256 devices in a mesh: gx: 8 (over x, z_hi), gy: 8 (over z_lo, core), gz: 4 (over y).
Axes of the slice: x: 4, y: 4, z: 8 (z_hi: 2, z_lo: 4; z = z_hi * 4 + z_lo), core: 2. Of those that a mesh axis runs over, the one named last changes fastest.
Arguments:
- section_state: float32 [25, 64, 128, 512], P(None, 'gx', 'gy', 'gz'), may hold values from -6 to 6
- step_start: float32 [25, 64, 128, 512], P(None, 'gx', 'gy', 'gz'), may hold values from -6 to 6
- weighted_sum: float32 [25, 64, 128, 512], P(None, 'gx', 'gy', 'gz'), may hold values from -6 to 6
- upwind_sign: int32 [3, 64, 128, 512], P(None, 'gx', 'gy', 'gz'), may hold values 0 or 1
Outputs:
- next_section: float32 [25, 64, 128, 512], P(None, 'gx', 'gy', 'gz')
- new_weighted: float32 [25, 64, 128, 512], P(None, 'gx', 'gy', 'gz')
The draws below stay inside these ranges and needn't reach their ends.
Inputs may be any that keep to these rules, and one draw needn't show every extreme that they name: upwind_sign[k] is 1 where the advection stencil along dimension k leans toward higher indices and 0 where it leans toward lower ones.
All inputs are finite; a program needn't handle non-finite values. No bound on the sum of `upwind_sign` on one device may be relied on, other than what follows from the above.
Results may differ from the reference program's by a relative error of at most 0.00002.
Values sent between devices are 32-bit elements; how exact they have to be, the bound alone decides.
A program may use at most 64 MiB of HBM per device.

```python
import jax
import jax.numpy as jnp

FIELDS = 25
NX = 64
NY = 128
NZ = 512


def touch_ends(array, rng, smallest, top_value):
    shape = array.shape
    spot = [jax.random.randint(jax.random.fold_in(rng, axis), (), 0, shape[axis]) for axis in range(len(shape))]
    array = array.at[tuple(spot)].set(smallest)
    longest = shape.index(max(shape))
    spot[longest] = (spot[longest] + 1) % shape[longest]
    return array.at[tuple(spot)].set(top_value)


def level_of(key, dims, cuts, least, high):
    loudness = 1.0
    for position, parts in cuts:
        draws = jax.random.uniform(jax.random.fold_in(jax.random.fold_in(key, 6), position), (parts,), jnp.float32, least / len(cuts), high / len(cuts))
        loudness = loudness * jnp.repeat(jnp.exp(draws), dims[position] // parts).reshape((-1,) + (1,) * (len(dims) - 1 - position))
    return loudness


def gaussian(key, dims, spread, limit, pieces=(), held_as=jnp.bfloat16):
    drawn = jax.random.normal(key, dims, jnp.float32) * spread
    if len(pieces) > 0:
        drawn = level_of(key, dims, pieces, -0.22, 0.18) * drawn
    return jnp.clip(drawn, min=-limit, max=limit).astype(held_as)


def setup_inputs(seed: int = 0) -> dict:
    keys = jax.random.split(jax.random.key(seed), 5)
    return {
        "section_state": gaussian(keys[0], (FIELDS, NX, NY, NZ), 1.0, 6.0, ((1, 8), (2, 8), (3, 4)), jnp.float32),
        "step_start": gaussian(keys[1], (FIELDS, NX, NY, NZ), 1.0, 6.0, ((1, 8), (2, 8), (3, 4)), jnp.float32),
        "weighted_sum": gaussian(keys[2], (FIELDS, NX, NY, NZ), 1.0, 6.0, ((1, 8), (2, 8), (3, 4)), jnp.float32),
        "upwind_sign": touch_ends((jax.random.randint(keys[3], (3, NX, NY, NZ), 0, 2) < 1).astype(jnp.int32), jax.random.fold_in(keys[3], 1), 0, 1),
    }


first_table = ((-2, 1.0), (-1, -8.0), (1, 8.0), (2, -1.0))
second_table = ((-2, -1.0), (-1, 16.0), (0, -30.0), (1, 16.0), (2, -1.0))
ahead_table = ((-1, -3.0), (0, -10.0), (1, 18.0), (2, -6.0), (3, 1.0))
behind_table = ((-3, -1.0), (-2, 6.0), (-1, -18.0), (0, 10.0), (1, 3.0))
smooth_table = ((-3, 1.0), (-2, -6.0), (-1, 15.0), (0, -20.0), (1, 15.0), (2, -6.0), (3, 1.0))
sym_pairs = ((0, 0), (0, 1), (0, 2), (1, 1), (1, 2), (2, 2))
kappa_one = 0.5
damping = 2.0
dissipation = 0.3
time_step = 0.25


def window(padded, extent, offset):
    return padded[3 + offset[0]:3 + offset[0] + extent[0], 3 + offset[1]:3 + offset[1] + extent[1], 3 + offset[2]:3 + offset[2] + extent[2]]


def stencil(padded, extent, axis_dim, weights, factor):
    summed = None
    for shift_by, weight in weights:
        offset = [0, 0, 0]
        offset[axis_dim] = shift_by
        addend = weight * window(padded, extent, offset)
        summed = addend if summed is None else summed + addend
    return summed * factor


def mixed_diff(padded, extent, dim_one, dim_two):
    summed = None
    for shift_a, weight_a in first_table:
        for shift_b, weight_b in first_table:
            offset = [0, 0, 0]
            offset[dim_one] = shift_a
            offset[dim_two] = shift_b
            addend = (weight_a * weight_b) * window(padded, extent, offset)
            summed = addend if summed is None else summed + addend
    return summed * (1.0 / 144.0)


def hessian(padded, extent):
    result = {}
    for i, j in sym_pairs:
        if i == j:
            result[(i, j)] = stencil(padded, extent, i, second_table, 1.0 / 12.0)
        else:
            result[(i, j)] = mixed_diff(padded, extent, i, j)
    return result


def field_rates(fields, upwind_sign):
    extent = upwind_sign.shape[1:]
    centre = [window(f, extent, (0, 0, 0)) for f in fields]

    def grad_of(which, k):
        return stencil(fields[which], extent, k, first_table, 1.0 / 12.0)

    grad_shift = [[grad_of(19 + m, k) for k in range(3)] for m in range(3)]
    grad_gamma = [[grad_of(14 + m, k) for k in range(3)] for m in range(3)]
    grad_trace = [grad_of(7, k) for k in range(3)]
    hess_chi = hessian(fields[0], extent)
    hess_lapse = hessian(fields[18], extent)
    hess_shift = [hessian(fields[19 + m], extent) for m in range(3)]
    lap_chi = hess_chi[(0, 0)] + hess_chi[(1, 1)] + hess_chi[(2, 2)]
    lap_lapse = hess_lapse[(0, 0)] + hess_lapse[(1, 1)] + hess_lapse[(2, 2)]
    diverge = grad_shift[0][0] + grad_shift[1][1] + grad_shift[2][2]
    local_rates = [(2.0 / 3.0) * (centre[7] - diverge)]
    for s, (i, j) in enumerate(sym_pairs):
        total_rate = -2.0 * centre[8 + s] + grad_shift[j][i] + grad_shift[i][j]
        if i == j:
            total_rate = total_rate - (2.0 / 3.0) * diverge
        local_rates.append(total_rate)
    local_rates.append(-lap_lapse + kappa_one * centre[17])
    ricci = []
    for s, (i, j) in enumerate(sym_pairs):
        lap_metric = stencil(fields[1 + s], extent, 0, second_table, 1.0 / 12.0)
        lap_metric = lap_metric + stencil(fields[1 + s], extent, 1, second_table, 1.0 / 12.0)
        lap_metric = lap_metric + stencil(fields[1 + s], extent, 2, second_table, 1.0 / 12.0)
        total_rate = -0.5 * lap_metric + 0.5 * (grad_gamma[j][i] + grad_gamma[i][j]) + 0.5 * hess_chi[(i, j)]
        if i == j:
            total_rate = total_rate + 0.5 * lap_chi
        ricci.append(total_rate)
    bare_curv = [ricci[s] - hess_lapse[sym_pairs[s]] for s in range(6)]
    trace_sum = bare_curv[0] + bare_curv[3] + bare_curv[5]
    for s, (i, j) in enumerate(sym_pairs):
        if i == j:
            local_rates.append(bare_curv[s] - (1.0 / 3.0) * trace_sum)
        else:
            local_rates.append(bare_curv[s])
    drive_terms = []
    for i in range(3):
        lap_shift = hess_shift[i][(0, 0)] + hess_shift[i][(1, 1)] + hess_shift[i][(2, 2)]
        grad_div = None
        for k in range(3):
            addend = hess_shift[k][(min(i, k), max(i, k))]
            grad_div = addend if grad_div is None else grad_div + addend
        drive_terms.append(-(4.0 / 3.0) * grad_trace[i] + lap_shift + (1.0 / 3.0) * grad_div)
    local_rates.extend(drive_terms)
    local_rates.append(0.5 * (ricci[0] + ricci[3] + ricci[5]) - 2.0 * kappa_one * centre[17])
    local_rates.append(-2.0 * centre[7])
    for i in range(3):
        local_rates.append(0.75 * centre[22 + i])
    for i in range(3):
        local_rates.append(drive_terms[i] - damping * centre[22 + i])
    shift_vec = [centre[19], centre[20], centre[21]]
    leaning = [upwind_sign[k] == 1 for k in range(3)]
    result = []
    for n, source in enumerate(local_rates):
        total_rate = source
        for k in range(3):
            forward = stencil(fields[n], extent, k, ahead_table, 1.0 / 12.0)
            behind = stencil(fields[n], extent, k, behind_table, 1.0 / 12.0)
            total_rate = total_rate + shift_vec[k] * jnp.where(leaning[k], forward, behind)
            total_rate = total_rate + (dissipation / 64.0) * stencil(fields[n], extent, k, smooth_table, 1.0)
        result.append(total_rate)
    return jnp.stack(result)


def reference(section_state, step_start, weighted_sum, upwind_sign):
    padded = jnp.pad(section_state, ((0, 0), (3, 3), (3, 3), (3, 3)), mode="wrap")
    fields = [padded[n] for n in range(padded.shape[0])]
    rates_all = field_rates(fields, upwind_sign)
    return step_start + (time_step / 2.0) * rates_all, weighted_sum + (time_step / 3.0) * rates_all
```

```python
import functools

import jax
import jax.numpy as jnp
from jax import lax
from jax.experimental import pallas as pl
from jax.experimental.pallas import tpu as pltpu
from jax.sharding import PartitionSpec as P

MESH = pl.DeviceIdType.MESH

special = (0, 18, 19, 20, 21)
early_runs = ((18, 4), (0, 1))
middle_runs = ((14, 4), (7, 1), (1, 6))
late_runs = ((8, 6), (22, 3))
runs = early_runs + middle_runs + late_runs
sym_pairs = ((0, 0), (0, 1), (0, 2), (1, 1), (1, 2), (2, 2))
kappa_one = 0.5
damping = 2.0
dissipation = 0.3
time_step = 0.25

LAYERS = 14
ROWS = 32


def first_diff(at):
    return ((at(-2) - at(2)) + 8.0 * (at(1) - at(-1))) * (1.0 / 12.0)


def second_diff(at):
    return (16.0 * (at(-1) + at(1)) - (at(-2) + at(2)) - 30.0 * at(0)) * (1.0 / 12.0)


def drift(at, odd_weight, even_weight):
    sums = [at(m) + at(-m) for m in (1, 2, 3)]
    gaps = [at(m) - at(-m) for m in (1, 2, 3)]
    odd = gaps[2] - 6.0 * gaps[1] + 21.0 * gaps[0]
    even = sums[2] - 6.0 * sums[1] + 15.0 * sums[0] - 20.0 * at(0)
    return odd_weight * odd + even_weight * even


def kernel(
    sizes,
    state,
    sign,
    rates,
    cells,
    wrap,
    lean,
    weights,
    diff_y,
    diff_z,
    y_out,
    y_in,
    z_out,
    z_in,
    y_out2,
    y_in2,
    z_out2,
    z_in2,
    x_sent,
    x_got,
    n_sent,
    n_got,
    local,
):
    here = {axis: lax.axis_index(axis) for axis in sizes}

    def beside(axis, step):
        return {axis: lax.rem(here[axis] + step + sizes[axis], sizes[axis])}

    barrier = pltpu.get_barrier_semaphore()
    for axis in sizes:
        for step in (1, -1):
            pl.semaphore_signal(barrier, inc=1, device_id=beside(axis, step), device_id_type=MESH)
    own = pltpu.make_async_copy(state, cells.at[:, pl.ds(3, 8), pl.ds(8, 16)], local.at[0])
    own.start()
    leaning = pltpu.make_async_copy(sign, lean, local.at[1])
    leaning.start()

    def x_copy(side, run):
        first, count = runs[run]
        return pltpu.make_async_remote_copy(
            src_ref=state.at[pl.ds(first, count), pl.ds(0 if side else 5, 3)],
            dst_ref=cells.at[pl.ds(first, count), pl.ds(11 if side else 0, 3), pl.ds(8, 16)],
            send_sem=x_sent.at[side, run],
            recv_sem=x_got.at[side, run],
            device_id=beside("gx", -1 if side else 1),
            device_id_type=MESH,
        )

    def n_copy(which, side):
        axis, out, got = (
            ("gy", y_out, y_in),
            ("gz", z_out, z_in),
            ("gy", y_out2, y_in2),
            ("gz", z_out2, z_in2),
        )[which]
        return pltpu.make_async_remote_copy(
            src_ref=out.at[side],
            dst_ref=got.at[side],
            send_sem=n_sent.at[which, side],
            recv_sem=n_got.at[which, side],
            device_id=beside(axis, -1 if side else 1),
            device_id_type=MESH,
        )

    def x_start(chosen):
        for run in chosen:
            for side in (0, 1):
                x_copy(side, run).start()

    def x_wait(chosen):
        for run in chosen:
            for side in (0, 1):
                x_copy(side, run).wait_recv()

    def n_start(which):
        for side in (0, 1):
            n_copy(which, side).start()

    def n_wait(which):
        for side in (0, 1):
            n_copy(which, side).wait_recv()

    at_early = range(len(early_runs))
    at_middle = range(len(early_runs), len(early_runs) + len(middle_runs))
    at_late = range(len(early_runs) + len(middle_runs), len(runs))

    pl.semaphore_wait(barrier, 2 * len(sizes))
    x_start(at_early)

    own.wait()
    leaning.wait()

    @pl.loop(0, 25)
    def _(f):
        for r in range(3):
            y_out[0, f, r] = cells[f, pl.ds(3, 8), 21 + r]
            y_out[1, f, r] = cells[f, pl.ds(3, 8), 8 + r]

    @pl.loop(0, 25)
    def _(f):
        turned = cells[f, pl.ds(3, 8), pl.ds(8, 16)].reshape(128, 128).T
        z_out[0, f] = turned[120:128]
        z_out[1, f] = turned[0:8]

    n_start(0)

    @pl.loop(0, 8)
    def _(i):
        for k in range(3):
            scaled = cells[19 + k, 3 + i, pl.ds(8, 16)] * (1.0 / 24.0)
            weights[k, i] = scaled
            weights[3 + k, i] = dissipation / 64.0 + jnp.where(lean[k, i] == 1, scaled, -scaled)

    n_start(1)
    x_start(at_middle)

    lane = lax.broadcasted_iota(jnp.int32, (16, 128), 1)
    lane8 = lax.broadcasted_iota(jnp.int32, (8, 128), 1)

    def along_z(field, layer, start, count):
        inside = cells[field, layer, pl.ds(start, count)]
        outside = wrap[field, layer, pl.ds(start, count)]
        lanes = lane if count == 16 else lane8

        def at(m):
            if m == 0:
                return inside
            if m > 0:
                return pltpu.roll(jnp.where(lanes < m, outside, inside), 128 - m, 1)
            return pltpu.roll(jnp.where(lanes >= 128 + m, outside, inside), -m, 1)

        return at

    def along_y(field, i):
        return lambda m: cells[field, 3 + i, pl.ds(8 + m, 16)]

    def along_x(field, i):
        return lambda m: cells[field, 3 + i + m, pl.ds(8, 16)]

    def turned_back(low, high):
        return jnp.concatenate([high, jnp.zeros((112, 128), jnp.float32), low], axis=0).T

    n_wait(0)

    @pl.loop(0, 25)
    def _(f):
        for r in range(3):
            cells[f, pl.ds(3, 8), 5 + r] = y_in[0, f, r]
            cells[f, pl.ds(3, 8), 24 + r] = y_in[1, f, r]

    n_wait(1)

    @pl.loop(0, 25)
    def _(f):
        wrap[f, pl.ds(3, 8), pl.ds(8, 16)] = turned_back(z_in[0, f], z_in[1, f]).reshape(8, 16, 128)

    x_wait(at_early)
    for n, f in enumerate(special):
        for q, layer in enumerate((1, 2, 11, 12)):
            y_out2[0, n, pl.ds(2 * q, 2)] = cells[f, layer, pl.ds(22, 2)]
            y_out2[1, n, pl.ds(2 * q, 2)] = cells[f, layer, pl.ds(8, 2)]
        turned = jnp.concatenate(
            [
                cells[f, pl.ds(1, 2), pl.ds(8, 16)].reshape(32, 128),
                cells[f, pl.ds(11, 2), pl.ds(8, 16)].reshape(32, 128),
                y_in[0, f, 1],
                y_in[0, f, 2],
                y_in[1, f, 0],
                y_in[1, f, 1],
                jnp.zeros((32, 128), jnp.float32),
            ],
            axis=0,
        ).T
        z_out2[0, n] = turned[120:128]
        z_out2[1, n] = turned[0:8]

    @pl.loop(0, 25)
    def _(f):
        @pl.loop(0, 8)
        def _(i):
            rates[f, i] = drift(along_y(f, i), weights[1, i], weights[4, i]) + drift(
                along_z(f, 3 + i, 8, 16), weights[2, i], weights[5, i]
            )

    n_start(2)
    n_start(3)
    x_start(at_late)

    def drift_x(first, count):
        @pl.loop(first, first + count)
        def _(f):
            @pl.loop(0, 8)
            def _(i):
                rates[f, i] += drift(along_x(f, i), weights[0, i], weights[3, i])

    for run in at_early:
        drift_x(*runs[run])

    n_wait(2)
    n_wait(3)
    for n, f in enumerate(special):
        for q, layer in enumerate((1, 2, 11, 12)):
            cells[f, layer, pl.ds(6, 2)] = y_in2[0, n, pl.ds(2 * q, 2)]
            cells[f, layer, pl.ds(24, 2)] = y_in2[1, n, pl.ds(2 * q, 2)]
        back = turned_back(z_in2[0, n], z_in2[1, n])
        wrap[f, pl.ds(1, 2), pl.ds(8, 16)] = back[0:32].reshape(2, 16, 128)
        wrap[f, pl.ds(11, 2), pl.ds(8, 16)] = back[32:64].reshape(2, 16, 128)
        for q, row in enumerate((6, 7, 24, 25)):
            wrap[f, pl.ds(3, 8), row] = back[64 + 8 * q : 72 + 8 * q]
        for layer in range(1, 13):
            diff_y[n, layer] = first_diff(lambda m: cells[f, layer, pl.ds(8 + m, 16)])
            diff_z[n, layer, pl.ds(8, 16)] = first_diff(along_z(f, layer, 8, 16))
        for layer in range(3, 11):
            diff_z[n, layer, pl.ds(0, 8)] = first_diff(along_z(f, layer, 0, 8))
            diff_z[n, layer, pl.ds(24, 8)] = first_diff(along_z(f, layer, 24, 8))

    for run in at_middle:
        x_wait([run])
        drift_x(*runs[run])

    @pl.loop(0, 8)
    def _(i):
        layer = 3 + i

        def centre(field):
            return cells[field, layer, pl.ds(8, 16)]

        def along(field, k):
            return (along_x(field, i), along_y(field, i), along_z(field, layer, 8, 16))[k]

        def grad(field, k):
            if field in special and k > 0:
                n = special.index(field)
                return diff_y[n, layer] if k == 1 else diff_z[n, layer, pl.ds(8, 16)]
            return first_diff(along(field, k))

        def hess(field, k, l):
            n = special.index(field)
            if k == l:
                return second_diff(along(field, k))
            if (k, l) == (0, 1):
                return first_diff(lambda m: diff_y[n, layer + m])
            if (k, l) == (0, 2):
                return first_diff(lambda m: diff_z[n, layer + m, pl.ds(8, 16)])
            return first_diff(lambda m: diff_z[n, layer, pl.ds(8 + m, 16)])

        def add(field, value):
            rates[field, i] += value

        grad_shift = [[grad(19 + m, k) for k in range(3)] for m in range(3)]
        diverge = grad_shift[0][0] + grad_shift[1][1] + grad_shift[2][2]
        add(0, 2.0 / 3.0 * (centre(7) - diverge))
        for s, (p, q) in enumerate(sym_pairs):
            value = -2.0 * centre(8 + s) + grad_shift[q][p] + grad_shift[p][q]
            if p == q:
                value = value - 2.0 / 3.0 * diverge
            add(1 + s, value)
        add(18, -2.0 * centre(7))
        for p in range(3):
            add(19 + p, 0.75 * centre(22 + p))
        hess_shift = [{pair: hess(19 + m, *pair) for pair in sym_pairs} for m in range(3)]
        for p in range(3):
            lap_shift = hess_shift[p][0, 0] + hess_shift[p][1, 1] + hess_shift[p][2, 2]
            grad_div = hess_shift[0][0, p] + hess_shift[1][min(1, p), max(1, p)] + hess_shift[2][p, 2]
            drive = -(4.0 / 3.0) * grad(7, p) + lap_shift + 1.0 / 3.0 * grad_div
            add(14 + p, drive)
            add(22 + p, drive - damping * centre(22 + p))
        hess_chi = {pair: hess(0, *pair) for pair in sym_pairs}
        hess_lapse = {pair: hess(18, *pair) for pair in sym_pairs}
        lap_chi = hess_chi[0, 0] + hess_chi[1, 1] + hess_chi[2, 2]
        lap_lapse = hess_lapse[0, 0] + hess_lapse[1, 1] + hess_lapse[2, 2]
        add(7, -lap_lapse + kappa_one * centre(17))
        grad_gamma = [[grad(14 + m, k) for k in range(3)] for m in range(3)]
        ricci = []
        for s, (p, q) in enumerate(sym_pairs):
            lap_metric = second_diff(along(1 + s, 0)) + second_diff(along(1 + s, 1)) + second_diff(along(1 + s, 2))
            value = -0.5 * lap_metric + 0.5 * (grad_gamma[q][p] + grad_gamma[p][q]) + 0.5 * hess_chi[p, q]
            if p == q:
                value = value + 0.5 * lap_chi
            ricci.append(value)
        bare = [ricci[s] - hess_lapse[pair] for s, pair in enumerate(sym_pairs)]
        trace = bare[0] + bare[3] + bare[5]
        for s, (p, q) in enumerate(sym_pairs):
            add(8 + s, bare[s] - 1.0 / 3.0 * trace if p == q else bare[s])
        add(17, 0.5 * (ricci[0] + ricci[3] + ricci[5]) - 2.0 * kappa_one * centre(17))

    for run in at_late:
        x_wait([run])
        drift_x(*runs[run])

    for run in range(len(runs)):
        for side in (0, 1):
            x_copy(side, run).wait_send()
    for which in range(4):
        for side in (0, 1):
            n_copy(which, side).wait_send()


def rates_of(sizes, state, sign):
    block = (8, 16, 128)
    f32 = jnp.float32
    return pl.pallas_call(
        functools.partial(kernel, sizes),
        out_shape=jax.ShapeDtypeStruct((25,) + block, f32),
        in_specs=[pl.BlockSpec(memory_space=pl.ANY)] * 2,
        out_specs=pl.BlockSpec(memory_space=pltpu.VMEM),
        scratch_shapes=[
            pltpu.VMEM((25, LAYERS, ROWS, 128), f32),
            pltpu.VMEM((25, LAYERS, ROWS, 128), f32),
            pltpu.VMEM((3,) + block, jnp.int32),
            pltpu.VMEM((6,) + block, f32),
            pltpu.VMEM((5, LAYERS, 16, 128), f32),
            pltpu.VMEM((5, LAYERS, ROWS, 128), f32),
            pltpu.VMEM((2, 25, 3, 8, 128), f32),
            pltpu.VMEM((2, 25, 3, 8, 128), f32),
            pltpu.VMEM((2, 25, 8, 128), f32),
            pltpu.VMEM((2, 25, 8, 128), f32),
            pltpu.VMEM((2, 5, 8, 128), f32),
            pltpu.VMEM((2, 5, 8, 128), f32),
            pltpu.VMEM((2, 5, 8, 128), f32),
            pltpu.VMEM((2, 5, 8, 128), f32),
            pltpu.SemaphoreType.DMA((2, len(runs))),
            pltpu.SemaphoreType.DMA((2, len(runs))),
            pltpu.SemaphoreType.DMA((4, 2)),
            pltpu.SemaphoreType.DMA((4, 2)),
            pltpu.SemaphoreType.DMA((2,)),
        ],
        compiler_params=pltpu.CompilerParams(
            collective_id=0, has_side_effects=True, vmem_limit_bytes=40 * 2**20
        ),
    )(state, sign)


def solution(mesh):
    placed = P(None, "gx", "gy", "gz")
    sizes = dict(mesh.shape)

    def on_device(section_state, step_start, weighted_sum, upwind_sign):
        rates = rates_of(sizes, section_state, upwind_sign)
        return step_start + time_step / 2.0 * rates, weighted_sum + time_step / 3.0 * rates

    return jax.shard_map(
        on_device, mesh=mesh, in_specs=(placed,) * 4, out_specs=(placed, placed), check_vma=False
    )
```

```python
import functools

import jax
import jax.numpy as jnp
from jax import lax
from jax.experimental import pallas as pl
from jax.experimental.pallas import tpu as pltpu
from jax.sharding import PartitionSpec as P

MESH = pl.DeviceIdType.MESH

special = (0, 18, 19, 20, 21)
early_runs = ((18, 4), (0, 1))
middle_runs = ((14, 4), (7, 1), (1, 6))
late_runs = ((8, 6), (22, 3))
runs = early_runs + middle_runs + late_runs
sym_pairs = ((0, 0), (0, 1), (0, 2), (1, 1), (1, 2), (2, 2))
kappa_one = 0.5
damping = 2.0
dissipation = 0.3
time_step = 0.25

LAYERS = 14
ROWS = 32


def first_diff(at):
    return ((at(-2) - at(2)) + 8.0 * (at(1) - at(-1))) * (1.0 / 12.0)


def second_diff(at):
    return (16.0 * (at(-1) + at(1)) - (at(-2) + at(2)) - 30.0 * at(0)) * (1.0 / 12.0)


def drift(at, odd_weight, even_weight):
    sums = [at(m) + at(-m) for m in (1, 2, 3)]
    gaps = [at(m) - at(-m) for m in (1, 2, 3)]
    odd = gaps[2] - 6.0 * gaps[1] + 21.0 * gaps[0]
    even = sums[2] - 6.0 * sums[1] + 15.0 * sums[0] - 20.0 * at(0)
    return odd_weight * odd + even_weight * even


def kernel(
    sizes,
    state,
    start,
    before,
    sign,
    ahead,
    after,
    rates,
    first_of,
    before_of,
    cells,
    wrap,
    lean,
    weights,
    diff_y,
    diff_z,
    y_out,
    y_in,
    z_out,
    z_in,
    y_out2,
    y_in2,
    z_out2,
    z_in2,
    x_sent,
    x_got,
    n_sent,
    n_got,
    local,
):
    here = {axis: lax.axis_index(axis) for axis in sizes}

    def beside(axis, step):
        return {axis: lax.rem(here[axis] + step + sizes[axis], sizes[axis])}

    barrier = pltpu.get_barrier_semaphore()
    for axis in sizes:
        for step in (1, -1):
            pl.semaphore_signal(barrier, inc=1, device_id=beside(axis, step), device_id_type=MESH)
    own = pltpu.make_async_copy(state, cells.at[:, pl.ds(3, 8), pl.ds(8, 16)], local.at[0])
    own.start()
    leaning = pltpu.make_async_copy(sign, lean, local.at[1])
    leaning.start()
    bases = [
        pltpu.make_async_copy(start, first_of, local.at[2]),
        pltpu.make_async_copy(before, before_of, local.at[3]),
    ]

    def x_copy(side, run):
        first, count = runs[run]
        return pltpu.make_async_remote_copy(
            src_ref=state.at[pl.ds(first, count), pl.ds(0 if side else 5, 3)],
            dst_ref=cells.at[pl.ds(first, count), pl.ds(11 if side else 0, 3), pl.ds(8, 16)],
            send_sem=x_sent.at[side, run],
            recv_sem=x_got.at[side, run],
            device_id=beside("gx", -1 if side else 1),
            device_id_type=MESH,
        )

    def n_copy(which, side):
        axis, out, got = (
            ("gy", y_out, y_in),
            ("gz", z_out, z_in),
            ("gy", y_out2, y_in2),
            ("gz", z_out2, z_in2),
        )[which]
        return pltpu.make_async_remote_copy(
            src_ref=out.at[side],
            dst_ref=got.at[side],
            send_sem=n_sent.at[which, side],
            recv_sem=n_got.at[which, side],
            device_id=beside(axis, -1 if side else 1),
            device_id_type=MESH,
        )

    def x_start(chosen):
        for run in chosen:
            for side in (0, 1):
                x_copy(side, run).start()

    def x_wait(chosen):
        for run in chosen:
            for side in (0, 1):
                x_copy(side, run).wait_recv()

    def n_start(which):
        for side in (0, 1):
            n_copy(which, side).start()

    def n_wait(which):
        for side in (0, 1):
            n_copy(which, side).wait_recv()

    at_early = list(range(len(early_runs)))
    at_middle = list(range(len(early_runs), len(early_runs) + len(middle_runs)))
    at_late = list(range(len(early_runs) + len(middle_runs), len(runs)))

    pl.semaphore_wait(barrier, 2 * len(sizes))
    x_start(at_early)

    own.wait()
    leaning.wait()

    @pl.loop(0, 25)
    def _(f):
        for r in range(3):
            y_out[0, f, r] = cells[f, pl.ds(3, 8), 21 + r]
            y_out[1, f, r] = cells[f, pl.ds(3, 8), 8 + r]

    @pl.loop(0, 25)
    def _(f):
        turned = cells[f, pl.ds(3, 8), pl.ds(8, 16)].reshape(128, 128).T
        z_out[0, f] = turned[120:128]
        z_out[1, f] = turned[0:8]

    n_start(0)

    @pl.loop(0, 8)
    def _(i):
        for k in range(3):
            scaled = cells[19 + k, 3 + i, pl.ds(8, 16)] * (1.0 / 24.0)
            weights[k, i] = scaled
            weights[3 + k, i] = dissipation / 64.0 + jnp.where(lean[k, i] == 1, scaled, -scaled)

    n_start(1)
    x_start(at_middle)

    lane = lax.broadcasted_iota(jnp.int32, (16, 128), 1)
    lane8 = lax.broadcasted_iota(jnp.int32, (8, 128), 1)

    def along_z(field, layer, start, count):
        inside = cells[field, layer, pl.ds(start, count)]
        outside = wrap[field, layer, pl.ds(start, count)]
        lanes = lane if count == 16 else lane8

        def at(m):
            if m == 0:
                return inside
            if m > 0:
                return pltpu.roll(jnp.where(lanes < m, outside, inside), 128 - m, 1)
            return pltpu.roll(jnp.where(lanes >= 128 + m, outside, inside), -m, 1)

        return at

    def along_y(field, i):
        return lambda m: cells[field, 3 + i, pl.ds(8 + m, 16)]

    def along_x(field, i):
        return lambda m: cells[field, 3 + i + m, pl.ds(8, 16)]

    def turned_back(low, high):
        return jnp.concatenate([high, jnp.zeros((112, 128), jnp.float32), low], axis=0).T

    for copy in bases:
        copy.start()
    n_wait(0)

    @pl.loop(0, 25)
    def _(f):
        for r in range(3):
            cells[f, pl.ds(3, 8), 5 + r] = y_in[0, f, r]
            cells[f, pl.ds(3, 8), 24 + r] = y_in[1, f, r]

    n_wait(1)

    @pl.loop(0, 25)
    def _(f):
        wrap[f, pl.ds(3, 8), pl.ds(8, 16)] = turned_back(z_in[0, f], z_in[1, f]).reshape(8, 16, 128)

    @pl.loop(0, 25)
    def _(f):
        @pl.loop(0, 8, unroll=4)
        def _(i):
            rates[f, i] = drift(along_y(f, i), weights[1, i], weights[4, i]) + drift(
                along_z(f, 3 + i, 8, 16), weights[2, i], weights[5, i]
            )

    x_wait(at_early)
    for n, f in enumerate(special):
        for q, layer in enumerate((1, 2, 11, 12)):
            y_out2[0, n, pl.ds(2 * q, 2)] = cells[f, layer, pl.ds(22, 2)]
            y_out2[1, n, pl.ds(2 * q, 2)] = cells[f, layer, pl.ds(8, 2)]
        turned = jnp.concatenate(
            [
                cells[f, pl.ds(1, 2), pl.ds(8, 16)].reshape(32, 128),
                cells[f, pl.ds(11, 2), pl.ds(8, 16)].reshape(32, 128),
                y_in[0, f, 1],
                y_in[0, f, 2],
                y_in[1, f, 0],
                y_in[1, f, 1],
                jnp.zeros((32, 128), jnp.float32),
            ],
            axis=0,
        ).T
        z_out2[0, n] = turned[120:128]
        z_out2[1, n] = turned[0:8]

    def drift_x(first, count):
        @pl.loop(first, first + count)
        def _(f):
            @pl.loop(0, 8, unroll=2)
            def _(i):
                rates[f, i] += drift(along_x(f, i), weights[0, i], weights[3, i])

    for run in at_early:
        drift_x(*runs[run])

    n_start(2)
    n_start(3)
    x_start(at_late)

    n_wait(2)
    n_wait(3)
    for n, f in enumerate(special):
        for q, layer in enumerate((1, 2, 11, 12)):
            cells[f, layer, pl.ds(6, 2)] = y_in2[0, n, pl.ds(2 * q, 2)]
            cells[f, layer, pl.ds(24, 2)] = y_in2[1, n, pl.ds(2 * q, 2)]
        back = turned_back(z_in2[0, n], z_in2[1, n])
        wrap[f, pl.ds(1, 2), pl.ds(8, 16)] = back[0:32].reshape(2, 16, 128)
        wrap[f, pl.ds(11, 2), pl.ds(8, 16)] = back[32:64].reshape(2, 16, 128)
        for q, row in enumerate((6, 7, 24, 25)):
            wrap[f, pl.ds(3, 8), row] = back[64 + 8 * q : 72 + 8 * q]
        for layer in range(1, 13):
            diff_y[n, layer] = first_diff(lambda m: cells[f, layer, pl.ds(8 + m, 16)])
            diff_z[n, layer, pl.ds(8, 16)] = first_diff(along_z(f, layer, 8, 16))
        for layer in range(3, 11):
            diff_z[n, layer, pl.ds(0, 8)] = first_diff(along_z(f, layer, 0, 8))
            diff_z[n, layer, pl.ds(24, 8)] = first_diff(along_z(f, layer, 24, 8))

    for run in at_middle:
        x_wait([run])
        drift_x(*runs[run])

    @pl.loop(0, 8)
    def _(i):
        layer = 3 + i

        def centre(field):
            return cells[field, layer, pl.ds(8, 16)]

        def along(field, k):
            return (along_x(field, i), along_y(field, i), along_z(field, layer, 8, 16))[k]

        def grad(field, k):
            if field in special and k > 0:
                n = special.index(field)
                return diff_y[n, layer] if k == 1 else diff_z[n, layer, pl.ds(8, 16)]
            return first_diff(along(field, k))

        def hess(field, k, l):
            n = special.index(field)
            if k == l:
                return second_diff(along(field, k))
            if (k, l) == (0, 1):
                return first_diff(lambda m: diff_y[n, layer + m])
            if (k, l) == (0, 2):
                return first_diff(lambda m: diff_z[n, layer + m, pl.ds(8, 16)])
            return first_diff(lambda m: diff_z[n, layer, pl.ds(8 + m, 16)])

        def add(field, value):
            rates[field, i] += value

        grad_shift = [[grad(19 + m, k) for k in range(3)] for m in range(3)]
        diverge = grad_shift[0][0] + grad_shift[1][1] + grad_shift[2][2]
        add(0, 2.0 / 3.0 * (centre(7) - diverge))
        for s, (p, q) in enumerate(sym_pairs):
            value = -2.0 * centre(8 + s) + grad_shift[q][p] + grad_shift[p][q]
            if p == q:
                value = value - 2.0 / 3.0 * diverge
            add(1 + s, value)
        add(18, -2.0 * centre(7))
        for p in range(3):
            add(19 + p, 0.75 * centre(22 + p))
        hess_shift = [{pair: hess(19 + m, *pair) for pair in sym_pairs} for m in range(3)]
        for p in range(3):
            lap_shift = hess_shift[p][0, 0] + hess_shift[p][1, 1] + hess_shift[p][2, 2]
            grad_div = hess_shift[0][0, p] + hess_shift[1][min(1, p), max(1, p)] + hess_shift[2][p, 2]
            drive = -(4.0 / 3.0) * grad(7, p) + lap_shift + 1.0 / 3.0 * grad_div
            add(14 + p, drive)
            add(22 + p, drive - damping * centre(22 + p))
        hess_chi = {pair: hess(0, *pair) for pair in sym_pairs}
        hess_lapse = {pair: hess(18, *pair) for pair in sym_pairs}
        lap_chi = hess_chi[0, 0] + hess_chi[1, 1] + hess_chi[2, 2]
        lap_lapse = hess_lapse[0, 0] + hess_lapse[1, 1] + hess_lapse[2, 2]
        add(7, -lap_lapse + kappa_one * centre(17))
        grad_gamma = [[grad(14 + m, k) for k in range(3)] for m in range(3)]
        ricci = []
        for s, (p, q) in enumerate(sym_pairs):
            lap_metric = second_diff(along(1 + s, 0)) + second_diff(along(1 + s, 1)) + second_diff(along(1 + s, 2))
            value = -0.5 * lap_metric + 0.5 * (grad_gamma[q][p] + grad_gamma[p][q]) + 0.5 * hess_chi[p, q]
            if p == q:
                value = value + 0.5 * lap_chi
            ricci.append(value)
        bare = [ricci[s] - hess_lapse[pair] for s, pair in enumerate(sym_pairs)]
        trace = bare[0] + bare[3] + bare[5]
        for s, (p, q) in enumerate(sym_pairs):
            add(8 + s, bare[s] - 1.0 / 3.0 * trace if p == q else bare[s])
        add(17, 0.5 * (ricci[0] + ricci[3] + ricci[5]) - 2.0 * kappa_one * centre(17))

    for copy in bases:
        copy.wait()

    def finish(f, i, value):
        ahead[f, i] = first_of[f, i] + time_step / 2.0 * value
        after[f, i] = before_of[f, i] + time_step / 3.0 * value

    for run in at_early + at_middle:
        first, count = runs[run]

        @pl.loop(first, first + count)
        def _(f):
            @pl.loop(0, 8, unroll=4)
            def _(i):
                finish(f, i, rates[f, i])

    for run in at_late:
        x_wait([run])
        first, count = runs[run]

        @pl.loop(first, first + count)
        def _(f):
            @pl.loop(0, 8, unroll=4)
            def _(i):
                finish(f, i, rates[f, i] + drift(along_x(f, i), weights[0, i], weights[3, i]))

    for run in range(len(runs)):
        for side in (0, 1):
            x_copy(side, run).wait_send()
    for which in range(4):
        for side in (0, 1):
            n_copy(which, side).wait_send()


def section_of(sizes, *arrays):
    block = (8, 16, 128)
    f32 = jnp.float32
    whole = jax.ShapeDtypeStruct((25,) + block, f32)
    return pl.pallas_call(
        functools.partial(kernel, sizes),
        out_shape=(whole, whole),
        in_specs=[pl.BlockSpec(memory_space=pltpu.HBM)] * 4,
        out_specs=[pl.BlockSpec(memory_space=pltpu.VMEM)] * 2,
        scratch_shapes=[
            pltpu.VMEM((25,) + block, f32),
            pltpu.VMEM((25,) + block, f32),
            pltpu.VMEM((25,) + block, f32),
            pltpu.VMEM((25, LAYERS, ROWS, 128), f32),
            pltpu.VMEM((25, LAYERS, ROWS, 128), f32),
            pltpu.VMEM((3,) + block, jnp.int32),
            pltpu.VMEM((6,) + block, f32),
            pltpu.VMEM((5, LAYERS, 16, 128), f32),
            pltpu.VMEM((5, LAYERS, ROWS, 128), f32),
            pltpu.VMEM((2, 25, 3, 8, 128), f32),
            pltpu.VMEM((2, 25, 3, 8, 128), f32),
            pltpu.VMEM((2, 25, 8, 128), f32),
            pltpu.VMEM((2, 25, 8, 128), f32),
            pltpu.VMEM((2, 5, 8, 128), f32),
            pltpu.VMEM((2, 5, 8, 128), f32),
            pltpu.VMEM((2, 5, 8, 128), f32),
            pltpu.VMEM((2, 5, 8, 128), f32),
            pltpu.SemaphoreType.DMA((2, len(runs))),
            pltpu.SemaphoreType.DMA((2, len(runs))),
            pltpu.SemaphoreType.DMA((4, 2)),
            pltpu.SemaphoreType.DMA((4, 2)),
            pltpu.SemaphoreType.DMA((4,)),
        ],
        compiler_params=pltpu.CompilerParams(
            collective_id=0, has_side_effects=True, vmem_limit_bytes=40 * 2**20
        ),
    )(*(pltpu.with_memory_space_constraint(x, pltpu.HBM) for x in arrays))


def put_out(ahead, after, ahead_out, after_out, sems):
    copies = [
        pltpu.make_async_copy(ahead, ahead_out, sems.at[0]),
        pltpu.make_async_copy(after, after_out, sems.at[1]),
    ]
    for copy in copies:
        copy.start()
    for copy in copies:
        copy.wait()


def solution(mesh):
    placed = P(None, "gx", "gy", "gz")
    sizes = dict(mesh.shape)

    def on_device(section_state, step_start, weighted_sum, upwind_sign):
        ahead, after = section_of(sizes, section_state, step_start, weighted_sum, upwind_sign)
        return pl.pallas_call(
            put_out,
            out_shape=(ahead, after),
            in_specs=[pl.BlockSpec(memory_space=pltpu.VMEM)] * 2,
            out_specs=[pl.BlockSpec(memory_space=pltpu.HBM)] * 2,
            scratch_shapes=[pltpu.SemaphoreType.DMA((2,))],
            compiler_params=pltpu.CompilerParams(vmem_limit_bytes=8 * 2**20),
        )(ahead, after)

    return jax.shard_map(
        on_device, mesh=mesh, in_specs=(placed,) * 4, out_specs=(placed, placed), check_vma=False
    )
```

```python
import functools

import jax
import jax.numpy as jnp
from jax import lax
from jax.experimental import pallas as pl
from jax.experimental.pallas import tpu as pltpu
from jax.sharding import PartitionSpec as P

MESH = pl.DeviceIdType.MESH

special = (0, 18, 19, 20, 21)
early_runs = ((14, 8), (0, 1))
middle_runs = ((1, 7),)
late_runs = ((8, 6), (22, 3))
runs = early_runs + middle_runs + late_runs
sym_pairs = ((0, 0), (0, 1), (0, 2), (1, 1), (1, 2), (2, 2))
kappa_one = 0.5
damping = 2.0
dissipation = 0.3
time_step = 0.25

LAYERS = 14
ROWS = 32
edge_layers = (1, 2, 11, 12)


def first_diff(at):
    return ((at(-2) - at(2)) + 8.0 * (at(1) - at(-1))) * (1.0 / 12.0)


def second_diff(at):
    return (16.0 * (at(-1) + at(1)) - (at(-2) + at(2)) - 30.0 * at(0)) * (1.0 / 12.0)


def drift(at, odd_weight, even_weight):
    sums = [at(m) + at(-m) for m in (1, 2, 3)]
    gaps = [at(m) - at(-m) for m in (1, 2, 3)]
    odd = gaps[2] - 6.0 * gaps[1] + 21.0 * gaps[0]
    even = sums[2] - 6.0 * sums[1] + 15.0 * sums[0] - 20.0 * at(0)
    return odd_weight * odd + even_weight * even


def kernel(
    sizes,
    state,
    start,
    before,
    sign,
    ahead,
    after,
    rates,
    first_of,
    before_of,
    cells,
    wrap,
    lean,
    weights,
    diff_y,
    diff_z,
    y_out,
    y_in,
    z_out,
    z_in,
    y_out2,
    y_in2,
    z_out2,
    z_in2,
    edge,
    x_sent,
    x_got,
    n_sent,
    n_got,
    local,
):
    here = {axis: lax.axis_index(axis) for axis in sizes}

    def beside(axis, step):
        return {axis: lax.rem(here[axis] + step + sizes[axis], sizes[axis])}

    barrier = pltpu.get_barrier_semaphore()
    for axis in sizes:
        for step in (1, -1):
            pl.semaphore_signal(barrier, inc=1, device_id=beside(axis, step), device_id_type=MESH)
    own = pltpu.make_async_copy(state, cells.at[:, pl.ds(3, 8), pl.ds(8, 16)], local.at[0])
    own.start()
    leaning = pltpu.make_async_copy(sign, lean, local.at[1])
    leaning.start()
    bases = [
        pltpu.make_async_copy(start, first_of, local.at[2]),
        pltpu.make_async_copy(before, before_of, local.at[3]),
    ]

    def x_copy(side, run):
        first, count = runs[run]
        return pltpu.make_async_remote_copy(
            src_ref=state.at[pl.ds(first, count), pl.ds(0 if side else 5, 3)],
            dst_ref=cells.at[pl.ds(first, count), pl.ds(11 if side else 0, 3), pl.ds(8, 16)],
            send_sem=x_sent.at[side, run],
            recv_sem=x_got.at[side, run],
            device_id=beside("gx", -1 if side else 1),
            device_id_type=MESH,
        )

    def n_copy(which, side):
        axis, out, got = (
            ("gy", y_out, y_in),
            ("gz", z_out, z_in),
            ("gy", y_out2, y_in2),
            ("gz", z_out2, z_in2),
        )[which]
        return pltpu.make_async_remote_copy(
            src_ref=out.at[side],
            dst_ref=got.at[side],
            send_sem=n_sent.at[which, side],
            recv_sem=n_got.at[which, side],
            device_id=beside(axis, -1 if side else 1),
            device_id_type=MESH,
        )

    def x_start(chosen):
        for run in chosen:
            for side in (0, 1):
                x_copy(side, run).start()

    def x_wait(chosen):
        for run in chosen:
            for side in (0, 1):
                x_copy(side, run).wait_recv()

    def n_start(which):
        for side in (0, 1):
            n_copy(which, side).start()

    def n_wait(which):
        for side in (0, 1):
            n_copy(which, side).wait_recv()

    at_early = list(range(len(early_runs)))
    at_middle = list(range(len(early_runs), len(early_runs) + len(middle_runs)))
    at_late = list(range(len(early_runs) + len(middle_runs), len(runs)))

    pl.semaphore_wait(barrier, 2 * len(sizes))
    x_start(at_early[:1])

    own.wait()
    leaning.wait()

    @pl.loop(0, 25)
    def _(f):
        for r in range(3):
            y_out[0, f, r] = cells[f, pl.ds(3, 8), 21 + r]
            y_out[1, f, r] = cells[f, pl.ds(3, 8), 8 + r]

    @pl.loop(0, 25)
    def _(f):
        turned = cells[f, pl.ds(3, 8), pl.ds(8, 16)].reshape(128, 128).T
        z_out[0, f] = turned[120:128]
        z_out[1, f] = turned[0:8]

    n_start(0)
    for f in special:
        for layer in edge_layers:
            cells[f, layer, pl.ds(0, 8)] = jnp.zeros((8, 128), jnp.float32)
            cells[f, layer, pl.ds(24, 8)] = jnp.zeros((8, 128), jnp.float32)
    edge[...] = jnp.zeros_like(edge)

    @pl.loop(0, 8)
    def _(i):
        for k in range(3):
            scaled = cells[19 + k, 3 + i, pl.ds(8, 16)] * (1.0 / 24.0)
            weights[k, i] = scaled
            weights[3 + k, i] = dissipation / 64.0 + jnp.where(lean[k, i] == 1, scaled, -scaled)

    n_start(1)
    low_half = lax.rem(here["gx"], 2) == 0
    held = at_late[1:]
    x_start([run for run in at_early[1:] + at_middle + at_late if run not in held])

    @pl.when(jnp.logical_not(low_half))
    def _():
        x_start(held)


    lane = lax.broadcasted_iota(jnp.int32, (16, 128), 1)
    lane8 = lax.broadcasted_iota(jnp.int32, (8, 128), 1)

    def along_z(field, layer, start, count):
        inside = cells[field, layer, pl.ds(start, count)]
        outside = wrap[field, layer, pl.ds(start, count)]
        lanes = lane if count == 16 else lane8

        def at(m):
            if m == 0:
                return inside
            if m > 0:
                return pltpu.roll(jnp.where(lanes < m, outside, inside), 128 - m, 1)
            return pltpu.roll(jnp.where(lanes >= 128 + m, outside, inside), -m, 1)

        return at

    def along_y(field, i):
        return lambda m: cells[field, 3 + i, pl.ds(8 + m, 16)]

    def along_x(field, i):
        return lambda m: cells[field, 3 + i + m, pl.ds(8, 16)]

    def turned_back(low, high):
        return jnp.concatenate([high, jnp.zeros((112, 128), jnp.float32), low], axis=0).T

    for copy in bases:
        copy.start()
    n_wait(0)

    @pl.loop(0, 25)
    def _(f):
        for r in range(3):
            cells[f, pl.ds(3, 8), 5 + r] = y_in[0, f, r]
            cells[f, pl.ds(3, 8), 24 + r] = y_in[1, f, r]

    n_wait(1)

    @pl.loop(0, 25)
    def _(f):
        wrap[f, pl.ds(3, 8), pl.ds(8, 16)] = turned_back(z_in[0, f], z_in[1, f]).reshape(8, 16, 128)

    @pl.loop(0, 25)
    def _(f):
        @pl.loop(0, 8, unroll=4)
        def _(i):
            rates[f, i] = drift(along_y(f, i), weights[1, i], weights[4, i]) + drift(
                along_z(f, 3 + i, 8, 16), weights[2, i], weights[5, i]
            )

    x_wait(at_early)

    def of_xy(n, layer, rows):
        if n == 0:
            return 0.5 * cells[0, layer, rows] - cells[18, layer, rows]
        return cells[18 + n, layer, rows]

    for n in range(3):
        for q, layer in enumerate(edge_layers):
            y_out2[0, n, pl.ds(2 * q, 2)] = of_xy(n, layer, pl.ds(22, 2))
            y_out2[1, n, pl.ds(2 * q, 2)] = of_xy(n, layer, pl.ds(8, 2))
    for n, f in enumerate(special):
        turned = jnp.concatenate(
            [
                cells[f, pl.ds(1, 2), pl.ds(8, 16)].reshape(32, 128),
                cells[f, pl.ds(11, 2), pl.ds(8, 16)].reshape(32, 128),
                y_in[0, f, 1],
                y_in[0, f, 2],
                y_in[1, f, 0],
                y_in[1, f, 1],
                jnp.zeros((32, 128), jnp.float32),
            ],
            axis=0,
        ).T
        z_out2[0, n] = turned[120:128]
        z_out2[1, n] = turned[0:8]

    def drift_x(first, count):
        @pl.loop(first, first + count)
        def _(f):
            @pl.loop(0, 8, unroll=2)
            def _(i):
                rates[f, i] += drift(along_x(f, i), weights[0, i], weights[3, i])

    for run in at_early:
        drift_x(*runs[run])

    n_start(2)

    @pl.when(low_half)
    def _():
        x_start(held)

    n_start(3)
    n_wait(3)
    for n, f in enumerate(special):
        back = turned_back(z_in2[0, n], z_in2[1, n])
        wrap[f, pl.ds(1, 2), pl.ds(8, 16)] = back[0:32].reshape(2, 16, 128)
        wrap[f, pl.ds(11, 2), pl.ds(8, 16)] = back[32:64].reshape(2, 16, 128)
        for q, row in enumerate((6, 7, 24, 25)):
            wrap[f, pl.ds(3, 8), row] = back[64 + 8 * q : 72 + 8 * q]
        for layer in range(1, 13):
            diff_y[n, layer] = first_diff(lambda m: cells[f, layer, pl.ds(8 + m, 16)])
            diff_z[n, layer, pl.ds(8, 16)] = first_diff(along_z(f, layer, 8, 16))
        for layer in range(3, 11):
            diff_z[n, layer, pl.ds(0, 8)] = first_diff(along_z(f, layer, 0, 8))
            diff_z[n, layer, pl.ds(24, 8)] = first_diff(along_z(f, layer, 24, 8))

    @pl.loop(0, 8)
    def _(i):
        layer = 3 + i

        def centre(field):
            return cells[field, layer, pl.ds(8, 16)]

        def along(field, k):
            return (along_x(field, i), along_y(field, i), along_z(field, layer, 8, 16))[k]

        def grad(field, k):
            if field in special and k > 0:
                n = special.index(field)
                return diff_y[n, layer] if k == 1 else diff_z[n, layer, pl.ds(8, 16)]
            return first_diff(along(field, k))

        def hess(field, k, l):
            n = special.index(field)
            if k == l:
                return second_diff(along(field, k))
            if (k, l) == (0, 1):
                return first_diff(lambda m: diff_y[n, layer + m])
            if (k, l) == (0, 2):
                return first_diff(lambda m: diff_z[n, layer + m, pl.ds(8, 16)])
            return first_diff(lambda m: diff_z[n, layer, pl.ds(8 + m, 16)])

        def add(field, value):
            rates[field, i] += value

        grad_shift = [[grad(19 + m, k) for k in range(3)] for m in range(3)]
        diverge = grad_shift[0][0] + grad_shift[1][1] + grad_shift[2][2]
        add(0, 2.0 / 3.0 * (centre(7) - diverge))
        for s, (p, q) in enumerate(sym_pairs):
            value = -2.0 * centre(8 + s) + grad_shift[q][p] + grad_shift[p][q]
            if p == q:
                value = value - 2.0 / 3.0 * diverge
            add(1 + s, value)
        add(18, -2.0 * centre(7))
        for p in range(3):
            add(19 + p, 0.75 * centre(22 + p))
        hess_shift = [{pair: hess(19 + m, *pair) for pair in sym_pairs} for m in range(3)]
        for p in range(3):
            lap_shift = hess_shift[p][0, 0] + hess_shift[p][1, 1] + hess_shift[p][2, 2]
            grad_div = hess_shift[0][0, p] + hess_shift[1][min(1, p), max(1, p)] + hess_shift[2][p, 2]
            drive = lap_shift + 1.0 / 3.0 * grad_div
            if p > 0:
                drive = drive - (4.0 / 3.0) * grad(7, p)
            add(14 + p, drive)
            add(22 + p, drive - damping * centre(22 + p))
        hess_chi = {pair: hess(0, *pair) for pair in sym_pairs}
        hess_lapse = {pair: hess(18, *pair) for pair in sym_pairs}
        lap_chi = hess_chi[0, 0] + hess_chi[1, 1] + hess_chi[2, 2]
        lap_lapse = hess_lapse[0, 0] + hess_lapse[1, 1] + hess_lapse[2, 2]
        add(7, -lap_lapse + kappa_one * centre(17))
        grad_gamma = [[grad(14 + m, k) for k in range(3)] for m in range(3)]
        ricci = []
        for s, (p, q) in enumerate(sym_pairs):
            lap_metric = second_diff(along(1 + s, 1)) + second_diff(along(1 + s, 2))
            value = -0.5 * lap_metric + 0.5 * (grad_gamma[q][p] + grad_gamma[p][q]) + 0.5 * hess_chi[p, q]
            if p == q:
                value = value + 0.5 * lap_chi
            ricci.append(value)
        bare = [ricci[s] - hess_lapse[pair] for s, pair in enumerate(sym_pairs)]
        trace = bare[0] + bare[3] + bare[5]
        for s, (p, q) in enumerate(sym_pairs):
            add(8 + s, bare[s] - 1.0 / 3.0 * trace if p == q else bare[s])
        add(17, 0.5 * (ricci[0] + ricci[3] + ricci[5]) - 2.0 * kappa_one * centre(17))

    x_wait(at_middle)
    for run in at_middle:
        drift_x(*runs[run])

    @pl.loop(0, 8)
    def _(i):
        bent = [-0.5 * second_diff(along_x(1 + s, i)) for s in range(6)]
        trace = bent[0] + bent[3] + bent[5]
        for s, (p, q) in enumerate(sym_pairs):
            rates[8 + s, i] += bent[s] - 1.0 / 3.0 * trace if p == q else bent[s]
        rates[17, i] += 0.5 * trace
        slope = -(4.0 / 3.0) * first_diff(along_x(7, i))
        rates[14, i] += slope
        rates[22, i] += slope

    for copy in bases:
        copy.wait()

    def finish(f, i, value):
        ahead[f, i] = first_of[f, i] + time_step / 2.0 * value
        after[f, i] = before_of[f, i] + time_step / 3.0 * value

    for run in at_early + at_middle:
        first, count = runs[run]

        @pl.loop(first, first + count)
        def _(f):
            @pl.loop(0, 8, unroll=4)
            def _(i):
                finish(f, i, rates[f, i])

    for run in at_late:
        x_wait([run])
        first, count = runs[run]

        @pl.loop(first, first + count)
        def _(f):
            @pl.loop(0, 8, unroll=4)
            def _(i):
                finish(f, i, rates[f, i] + drift(along_x(f, i), weights[0, i], weights[3, i]))

    n_wait(2)

    def corner(n):
        for q in range(4):
            edge[n, q, pl.ds(6, 2)] = y_in2[0, n, pl.ds(2 * q, 2)]
            edge[n, q, pl.ds(24, 2)] = y_in2[1, n, pl.ds(2 * q, 2)]
        outer, inner, beyond, last = [
            first_diff(lambda m: edge[n, q, pl.ds(8 + m, 16)]) * (1.0 / 12.0) for q in range(4)
        ]
        return ((0, outer - 8.0 * inner), (1, inner), (6, -beyond), (7, 8.0 * beyond - last))

    for n, (fields, factor) in enumerate((((9,), 1.0), ((15, 23), 1.0 / 3.0), ((14, 22), 1.0 / 3.0))):
        for i, value in corner(n):
            for f in fields:
                ahead[f, i] += (time_step / 2.0 * factor) * value
                after[f, i] += (time_step / 3.0 * factor) * value

    for run in range(len(runs)):
        for side in (0, 1):
            x_copy(side, run).wait_send()
    for which in range(4):
        for side in (0, 1):
            n_copy(which, side).wait_send()


def section_of(sizes, *arrays):
    block = (8, 16, 128)
    f32 = jnp.float32
    whole = jax.ShapeDtypeStruct((25,) + block, f32)
    return pl.pallas_call(
        functools.partial(kernel, sizes),
        out_shape=(whole, whole),
        in_specs=[pl.BlockSpec(memory_space=pltpu.HBM)] * 4,
        out_specs=[pl.BlockSpec(memory_space=pltpu.VMEM)] * 2,
        scratch_shapes=[
            pltpu.VMEM((25,) + block, f32),
            pltpu.VMEM((25,) + block, f32),
            pltpu.VMEM((25,) + block, f32),
            pltpu.VMEM((25, LAYERS, ROWS, 128), f32),
            pltpu.VMEM((25, LAYERS, ROWS, 128), f32),
            pltpu.VMEM((3,) + block, jnp.int32),
            pltpu.VMEM((6,) + block, f32),
            pltpu.VMEM((5, LAYERS, 16, 128), f32),
            pltpu.VMEM((5, LAYERS, ROWS, 128), f32),
            pltpu.VMEM((2, 25, 3, 8, 128), f32),
            pltpu.VMEM((2, 25, 3, 8, 128), f32),
            pltpu.VMEM((2, 25, 8, 128), f32),
            pltpu.VMEM((2, 25, 8, 128), f32),
            pltpu.VMEM((2, 3, 8, 128), f32),
            pltpu.VMEM((2, 3, 8, 128), f32),
            pltpu.VMEM((2, 5, 8, 128), f32),
            pltpu.VMEM((2, 5, 8, 128), f32),
            pltpu.VMEM((3, 4, ROWS, 128), f32),
            pltpu.SemaphoreType.DMA((2, len(runs))),
            pltpu.SemaphoreType.DMA((2, len(runs))),
            pltpu.SemaphoreType.DMA((4, 2)),
            pltpu.SemaphoreType.DMA((4, 2)),
            pltpu.SemaphoreType.DMA((4,)),
        ],
        compiler_params=pltpu.CompilerParams(
            collective_id=0, has_side_effects=True, vmem_limit_bytes=40 * 2**20
        ),
    )(*(pltpu.with_memory_space_constraint(x, pltpu.HBM) for x in arrays))


def put_out(ahead, after, ahead_out, after_out, sems):
    copies = [
        pltpu.make_async_copy(ahead, ahead_out, sems.at[0]),
        pltpu.make_async_copy(after, after_out, sems.at[1]),
    ]
    for copy in copies:
        copy.start()
    for copy in copies:
        copy.wait()


def solution(mesh):
    placed = P(None, "gx", "gy", "gz")
    sizes = dict(mesh.shape)

    def on_device(section_state, step_start, weighted_sum, upwind_sign):
        ahead, after = section_of(sizes, section_state, step_start, weighted_sum, upwind_sign)
        return pl.pallas_call(
            put_out,
            out_shape=(ahead, after),
            in_specs=[pl.BlockSpec(memory_space=pltpu.VMEM)] * 2,
            out_specs=[pl.BlockSpec(memory_space=pltpu.HBM)] * 2,
            scratch_shapes=[pltpu.SemaphoreType.DMA((2,))],
            compiler_params=pltpu.CompilerParams(vmem_limit_bytes=8 * 2**20),
        )(ahead, after)

    return jax.shard_map(
        on_device, mesh=mesh, in_specs=(placed,) * 4, out_specs=(placed, placed), check_vma=False
    )
```

```python
import functools

import jax
import jax.numpy as jnp
from jax import lax
from jax.experimental import pallas as pl
from jax.experimental.pallas import tpu as pltpu
from jax.sharding import PartitionSpec as P

MESH = pl.DeviceIdType.MESH

special = (0, 18, 19, 20, 21)
early_runs = ((14, 8), (0, 1))
middle_runs = ((1, 7),)
late_runs = ((8, 6), (22, 3))
runs = early_runs + middle_runs + late_runs
sym_pairs = ((0, 0), (0, 1), (0, 2), (1, 1), (1, 2), (2, 2))
kappa_one = 0.5
damping = 2.0
dissipation = 0.3
time_step = 0.25

LAYERS = 14
ROWS = 32
edge_layers = (1, 2, 11, 12)
y_first = ((0, 8, 0), (14, 8, 8))
y_rest = ((8, 6, 16), (22, 3, 22))


def first_diff(at):
    return ((at(-2) - at(2)) + 8.0 * (at(1) - at(-1))) * (1.0 / 12.0)


def second_diff(at):
    return (16.0 * (at(-1) + at(1)) - (at(-2) + at(2)) - 30.0 * at(0)) * (1.0 / 12.0)


def drift(at, odd_weight, even_weight):
    sums = [at(m) + at(-m) for m in (1, 2, 3)]
    gaps = [at(m) - at(-m) for m in (1, 2, 3)]
    odd = gaps[2] - 6.0 * gaps[1] + 21.0 * gaps[0]
    even = sums[2] - 6.0 * sums[1] + 15.0 * sums[0] - 20.0 * at(0)
    return odd_weight * odd + even_weight * even


def kernel(
    sizes,
    state,
    start,
    before,
    sign,
    ahead,
    after,
    rates,
    first_of,
    before_of,
    cells,
    wrap,
    lean,
    weights,
    diff_y,
    diff_z,
    y_out,
    y_in,
    z_out,
    z_in,
    y_out2,
    y_in2,
    z_out2,
    z_in2,
    edge,
    x_sent,
    x_got,
    n_sent,
    n_got,
    local,
):
    here = {axis: lax.axis_index(axis) for axis in sizes}

    def beside(axis, step):
        return {axis: lax.rem(here[axis] + step + sizes[axis], sizes[axis])}

    barrier = pltpu.get_barrier_semaphore()
    for axis in sizes:
        for step in (1, -1):
            pl.semaphore_signal(barrier, inc=1, device_id=beside(axis, step), device_id_type=MESH)
    own = pltpu.make_async_copy(state, cells.at[:, pl.ds(3, 8), pl.ds(8, 16)], local.at[0])
    own.start()
    leaning = pltpu.make_async_copy(sign, lean, local.at[1])
    leaning.start()
    bases = [
        pltpu.make_async_copy(start, first_of, local.at[2]),
        pltpu.make_async_copy(before, before_of, local.at[3]),
    ]

    def x_copy(side, run):
        first, count = runs[run]
        return pltpu.make_async_remote_copy(
            src_ref=state.at[pl.ds(first, count), pl.ds(0 if side else 5, 3)],
            dst_ref=cells.at[pl.ds(first, count), pl.ds(11 if side else 0, 3), pl.ds(8, 16)],
            send_sem=x_sent.at[side, run],
            recv_sem=x_got.at[side, run],
            device_id=beside("gx", -1 if side else 1),
            device_id_type=MESH,
        )

    def n_copy(which, side):
        axis, out, got = (
            ("gy", y_out.at[side, pl.ds(0, 16)], y_in.at[side, pl.ds(0, 16)]),
            ("gz", z_out.at[side], z_in.at[side]),
            ("gy", y_out2.at[side], y_in2.at[side]),
            ("gz", z_out2.at[side], z_in2.at[side]),
            ("gy", y_out.at[side, pl.ds(16, 9)], y_in.at[side, pl.ds(16, 9)]),
        )[which]
        return pltpu.make_async_remote_copy(
            src_ref=out,
            dst_ref=got,
            send_sem=n_sent.at[which, side],
            recv_sem=n_got.at[which, side],
            device_id=beside(axis, -1 if side else 1),
            device_id_type=MESH,
        )

    def x_start(chosen):
        for run in chosen:
            for side in (0, 1):
                x_copy(side, run).start()

    def x_wait(chosen):
        for run in chosen:
            for side in (0, 1):
                x_copy(side, run).wait_recv()

    def x_left(chosen):
        for run in chosen:
            for side in (0, 1):
                x_copy(side, run).wait_send()

    def n_start(which):
        for side in (0, 1):
            n_copy(which, side).start()

    def n_wait(which):
        for side in (0, 1):
            n_copy(which, side).wait_recv()

    at_early = list(range(len(early_runs)))
    at_middle = list(range(len(early_runs), len(early_runs) + len(middle_runs)))
    at_late = list(range(len(early_runs) + len(middle_runs), len(runs)))

    pl.semaphore_wait(barrier, 2 * len(sizes))
    x_start(at_early[:1])

    own.wait()
    leaning.wait()

    for first, count, at in y_first + y_rest:

        @pl.loop(first, first + count)
        def _(f):
            for r in range(3):
                y_out[0, f - first + at, r] = cells[f, pl.ds(3, 8), 21 + r]
                y_out[1, f - first + at, r] = cells[f, pl.ds(3, 8), 8 + r]

    @pl.loop(0, 25)
    def _(f):
        turned = cells[f, pl.ds(3, 8), pl.ds(8, 16)].reshape(128, 128).T
        z_out[0, f] = turned[120:128]
        z_out[1, f] = turned[0:8]

    n_start(0)
    for f in special:
        for layer in edge_layers:
            cells[f, layer, pl.ds(0, 8)] = jnp.zeros((8, 128), jnp.float32)
            cells[f, layer, pl.ds(24, 8)] = jnp.zeros((8, 128), jnp.float32)
    edge[...] = jnp.zeros_like(edge)

    @pl.loop(0, 8)
    def _(i):
        for k in range(3):
            scaled = cells[19 + k, 3 + i, pl.ds(8, 16)] * (1.0 / 24.0)
            weights[k, i] = scaled
            weights[3 + k, i] = dissipation / 64.0 + jnp.where(lean[k, i] == 1, scaled, -scaled)

    n_start(1)
    low_half = lax.rem(here["gx"], 2) == 0

    @pl.when(low_half)
    def _():
        n_start(4)

    held = at_late[1:]
    x_start([run for run in at_early[1:] + at_middle + at_late if run not in held])

    @pl.when(jnp.logical_not(low_half))
    def _():
        x_start(held)


    lane = lax.broadcasted_iota(jnp.int32, (16, 128), 1)
    lane8 = lax.broadcasted_iota(jnp.int32, (8, 128), 1)

    def along_z(field, layer, start, count):
        inside = cells[field, layer, pl.ds(start, count)]
        outside = wrap[field, layer, pl.ds(start, count)]
        lanes = lane if count == 16 else lane8

        def at(m):
            if m == 0:
                return inside
            if m > 0:
                return pltpu.roll(jnp.where(lanes < m, outside, inside), 128 - m, 1)
            return pltpu.roll(jnp.where(lanes >= 128 + m, outside, inside), -m, 1)

        return at

    def along_y(field, i):
        return lambda m: cells[field, 3 + i, pl.ds(8 + m, 16)]

    def along_x(field, i):
        return lambda m: cells[field, 3 + i + m, pl.ds(8, 16)]

    def turned_back(low, high):
        return jnp.concatenate([high, jnp.zeros((112, 128), jnp.float32), low], axis=0).T

    for copy in bases:
        copy.start()
    n_wait(0)

    def y_place(parts):
        for first, count, at in parts:

            @pl.loop(first, first + count)
            def _(f):
                for r in range(3):
                    cells[f, pl.ds(3, 8), 5 + r] = y_in[0, f - first + at, r]
                    cells[f, pl.ds(3, 8), 24 + r] = y_in[1, f - first + at, r]

    y_place(y_first)

    n_wait(1)

    @pl.loop(0, 25)
    def _(f):
        wrap[f, pl.ds(3, 8), pl.ds(8, 16)] = turned_back(z_in[0, f], z_in[1, f]).reshape(8, 16, 128)

    for first, count, _ in y_first:

        @pl.loop(first, first + count)
        def _(f):
            @pl.loop(0, 8, unroll=4)
            def _(i):
                rates[f, i] = drift(along_y(f, i), weights[1, i], weights[4, i]) + drift(
                    along_z(f, 3 + i, 8, 16), weights[2, i], weights[5, i]
                )

    for first, count, _ in y_rest:

        @pl.loop(first, first + count)
        def _(f):
            @pl.loop(0, 8, unroll=4)
            def _(i):
                rates[f, i] = drift(along_z(f, 3 + i, 8, 16), weights[2, i], weights[5, i])

    x_wait(at_early)

    def of_xy(n, layer, rows):
        if n == 0:
            return 0.5 * cells[0, layer, rows] - cells[18, layer, rows]
        return cells[18 + n, layer, rows]

    for n in range(3):
        for q, layer in enumerate(edge_layers):
            y_out2[0, n, pl.ds(2 * q, 2)] = of_xy(n, layer, pl.ds(22, 2))
            y_out2[1, n, pl.ds(2 * q, 2)] = of_xy(n, layer, pl.ds(8, 2))
    for n, f in enumerate(special):
        y_at = f - 6 if f else 0
        turned = jnp.concatenate(
            [
                cells[f, pl.ds(1, 2), pl.ds(8, 16)].reshape(32, 128),
                cells[f, pl.ds(11, 2), pl.ds(8, 16)].reshape(32, 128),
                y_in[0, y_at, 1],
                y_in[0, y_at, 2],
                y_in[1, y_at, 0],
                y_in[1, y_at, 1],
                jnp.zeros((32, 128), jnp.float32),
            ],
            axis=0,
        ).T
        z_out2[0, n] = turned[120:128]
        z_out2[1, n] = turned[0:8]

    def drift_x(first, count):
        @pl.loop(first, first + count)
        def _(f):
            @pl.loop(0, 8, unroll=2)
            def _(i):
                rates[f, i] += drift(along_x(f, i), weights[0, i], weights[3, i])

    for run in at_early:
        drift_x(*runs[run])

    n_start(2)

    @pl.when(low_half)
    def _():
        x_start(held)

    n_start(3)
    n_wait(3)
    for n, f in enumerate(special):
        back = turned_back(z_in2[0, n], z_in2[1, n])
        wrap[f, pl.ds(1, 2), pl.ds(8, 16)] = back[0:32].reshape(2, 16, 128)
        wrap[f, pl.ds(11, 2), pl.ds(8, 16)] = back[32:64].reshape(2, 16, 128)
        for q, row in enumerate((6, 7, 24, 25)):
            wrap[f, pl.ds(3, 8), row] = back[64 + 8 * q : 72 + 8 * q]
        for layer in range(1, 13):
            diff_y[n, layer] = first_diff(lambda m: cells[f, layer, pl.ds(8 + m, 16)])
            diff_z[n, layer, pl.ds(8, 16)] = first_diff(along_z(f, layer, 8, 16))
        for layer in range(3, 11):
            diff_z[n, layer, pl.ds(0, 8)] = first_diff(along_z(f, layer, 0, 8))
            diff_z[n, layer, pl.ds(24, 8)] = first_diff(along_z(f, layer, 24, 8))

    @pl.loop(0, 8)
    def _(i):
        layer = 3 + i

        def centre(field):
            return cells[field, layer, pl.ds(8, 16)]

        def along(field, k):
            return (along_x(field, i), along_y(field, i), along_z(field, layer, 8, 16))[k]

        def grad(field, k):
            if field in special and k > 0:
                n = special.index(field)
                return diff_y[n, layer] if k == 1 else diff_z[n, layer, pl.ds(8, 16)]
            return first_diff(along(field, k))

        def hess(field, k, l):
            n = special.index(field)
            if k == l:
                return second_diff(along(field, k))
            if (k, l) == (0, 1):
                return first_diff(lambda m: diff_y[n, layer + m])
            if (k, l) == (0, 2):
                return first_diff(lambda m: diff_z[n, layer + m, pl.ds(8, 16)])
            return first_diff(lambda m: diff_z[n, layer, pl.ds(8 + m, 16)])

        def add(field, value):
            rates[field, i] += value

        grad_shift = [[grad(19 + m, k) for k in range(3)] for m in range(3)]
        diverge = grad_shift[0][0] + grad_shift[1][1] + grad_shift[2][2]
        add(0, 2.0 / 3.0 * (centre(7) - diverge))
        for s, (p, q) in enumerate(sym_pairs):
            value = -2.0 * centre(8 + s) + grad_shift[q][p] + grad_shift[p][q]
            if p == q:
                value = value - 2.0 / 3.0 * diverge
            add(1 + s, value)
        add(18, -2.0 * centre(7))
        for p in range(3):
            add(19 + p, 0.75 * centre(22 + p))
        hess_shift = [{pair: hess(19 + m, *pair) for pair in sym_pairs} for m in range(3)]
        for p in range(3):
            lap_shift = hess_shift[p][0, 0] + hess_shift[p][1, 1] + hess_shift[p][2, 2]
            grad_div = hess_shift[0][0, p] + hess_shift[1][min(1, p), max(1, p)] + hess_shift[2][p, 2]
            drive = lap_shift + 1.0 / 3.0 * grad_div
            if p > 0:
                drive = drive - (4.0 / 3.0) * grad(7, p)
            add(14 + p, drive)
            add(22 + p, drive - damping * centre(22 + p))
        hess_chi = {pair: hess(0, *pair) for pair in sym_pairs}
        hess_lapse = {pair: hess(18, *pair) for pair in sym_pairs}
        lap_chi = hess_chi[0, 0] + hess_chi[1, 1] + hess_chi[2, 2]
        lap_lapse = hess_lapse[0, 0] + hess_lapse[1, 1] + hess_lapse[2, 2]
        add(7, -lap_lapse + kappa_one * centre(17))
        grad_gamma = [[grad(14 + m, k) for k in range(3)] for m in range(3)]
        ricci = []
        for s, (p, q) in enumerate(sym_pairs):
            lap_metric = second_diff(along(1 + s, 1)) + second_diff(along(1 + s, 2))
            value = -0.5 * lap_metric + 0.5 * (grad_gamma[q][p] + grad_gamma[p][q]) + 0.5 * hess_chi[p, q]
            if p == q:
                value = value + 0.5 * lap_chi
            ricci.append(value)
        bare = [ricci[s] - hess_lapse[pair] for s, pair in enumerate(sym_pairs)]
        trace = bare[0] + bare[3] + bare[5]
        for s, (p, q) in enumerate(sym_pairs):
            add(8 + s, bare[s] - 1.0 / 3.0 * trace if p == q else bare[s])
        add(17, 0.5 * (ricci[0] + ricci[3] + ricci[5]) - 2.0 * kappa_one * centre(17))

    x_wait(at_middle)
    for run in at_middle:
        drift_x(*runs[run])

    @pl.loop(0, 8)
    def _(i):
        bent = [-0.5 * second_diff(along_x(1 + s, i)) for s in range(6)]
        trace = bent[0] + bent[3] + bent[5]
        for s, (p, q) in enumerate(sym_pairs):
            rates[8 + s, i] += bent[s] - 1.0 / 3.0 * trace if p == q else bent[s]
        rates[17, i] += 0.5 * trace
        slope = -(4.0 / 3.0) * first_diff(along_x(7, i))
        rates[14, i] += slope
        rates[22, i] += slope

    for copy in bases:
        copy.wait()

    def finish(f, i, value):
        ahead[f, i] = first_of[f, i] + time_step / 2.0 * value
        after[f, i] = before_of[f, i] + time_step / 3.0 * value

    for run in at_early + at_middle:
        first, count = runs[run]

        @pl.loop(first, first + count)
        def _(f):
            @pl.loop(0, 8, unroll=4)
            def _(i):
                finish(f, i, rates[f, i])

    @pl.when(jnp.logical_not(low_half))
    def _():
        x_left(at_early + at_middle + at_late[:1])
        n_start(4)

    n_wait(4)
    y_place(y_rest)
    for first, count, _ in y_rest:

        @pl.loop(first, first + count)
        def _(f):
            @pl.loop(0, 8, unroll=4)
            def _(i):
                rates[f, i] += drift(along_y(f, i), weights[1, i], weights[4, i])

    for run in at_late:
        x_wait([run])
        first, count = runs[run]

        @pl.loop(first, first + count)
        def _(f):
            @pl.loop(0, 8, unroll=4)
            def _(i):
                finish(f, i, rates[f, i] + drift(along_x(f, i), weights[0, i], weights[3, i]))

    n_wait(2)

    def corner(n):
        for q in range(4):
            edge[n, q, pl.ds(6, 2)] = y_in2[0, n, pl.ds(2 * q, 2)]
            edge[n, q, pl.ds(24, 2)] = y_in2[1, n, pl.ds(2 * q, 2)]
        outer, inner, beyond, last = [
            first_diff(lambda m: edge[n, q, pl.ds(8 + m, 16)]) * (1.0 / 12.0) for q in range(4)
        ]
        return ((0, outer - 8.0 * inner), (1, inner), (6, -beyond), (7, 8.0 * beyond - last))

    for n, (fields, factor) in enumerate((((9,), 1.0), ((15, 23), 1.0 / 3.0), ((14, 22), 1.0 / 3.0))):
        for i, value in corner(n):
            for f in fields:
                ahead[f, i] += (time_step / 2.0 * factor) * value
                after[f, i] += (time_step / 3.0 * factor) * value

    @pl.when(low_half)
    def _():
        x_left(at_early + at_middle + at_late[:1])

    x_left([run for run in range(len(runs)) if run not in at_early + at_middle + at_late[:1]])
    for which in range(5):
        for side in (0, 1):
            n_copy(which, side).wait_send()


def section_of(sizes, *arrays):
    block = (8, 16, 128)
    f32 = jnp.float32
    whole = jax.ShapeDtypeStruct((25,) + block, f32)
    return pl.pallas_call(
        functools.partial(kernel, sizes),
        out_shape=(whole, whole),
        in_specs=[pl.BlockSpec(memory_space=pltpu.HBM)] * 4,
        out_specs=[pl.BlockSpec(memory_space=pltpu.VMEM)] * 2,
        scratch_shapes=[
            pltpu.VMEM((25,) + block, f32),
            pltpu.VMEM((25,) + block, f32),
            pltpu.VMEM((25,) + block, f32),
            pltpu.VMEM((25, LAYERS, ROWS, 128), f32),
            pltpu.VMEM((25, LAYERS, ROWS, 128), f32),
            pltpu.VMEM((3,) + block, jnp.int32),
            pltpu.VMEM((6,) + block, f32),
            pltpu.VMEM((5, LAYERS, 16, 128), f32),
            pltpu.VMEM((5, LAYERS, ROWS, 128), f32),
            pltpu.VMEM((2, 25, 3, 8, 128), f32),
            pltpu.VMEM((2, 25, 3, 8, 128), f32),
            pltpu.VMEM((2, 25, 8, 128), f32),
            pltpu.VMEM((2, 25, 8, 128), f32),
            pltpu.VMEM((2, 3, 8, 128), f32),
            pltpu.VMEM((2, 3, 8, 128), f32),
            pltpu.VMEM((2, 5, 8, 128), f32),
            pltpu.VMEM((2, 5, 8, 128), f32),
            pltpu.VMEM((3, 4, ROWS, 128), f32),
            pltpu.SemaphoreType.DMA((2, len(runs))),
            pltpu.SemaphoreType.DMA((2, len(runs))),
            pltpu.SemaphoreType.DMA((5, 2)),
            pltpu.SemaphoreType.DMA((5, 2)),
            pltpu.SemaphoreType.DMA((4,)),
        ],
        compiler_params=pltpu.CompilerParams(
            collective_id=0, has_side_effects=True, vmem_limit_bytes=40 * 2**20
        ),
    )(*(pltpu.with_memory_space_constraint(x, pltpu.HBM) for x in arrays))


def put_out(ahead, after, ahead_out, after_out, sems):
    copies = [
        pltpu.make_async_copy(ahead, ahead_out, sems.at[0]),
        pltpu.make_async_copy(after, after_out, sems.at[1]),
    ]
    for copy in copies:
        copy.start()
    for copy in copies:
        copy.wait()


def solution(mesh):
    placed = P(None, "gx", "gy", "gz")
    sizes = dict(mesh.shape)

    def on_device(section_state, step_start, weighted_sum, upwind_sign):
        ahead, after = section_of(sizes, section_state, step_start, weighted_sum, upwind_sign)
        return pl.pallas_call(
            put_out,
            out_shape=(ahead, after),
            in_specs=[pl.BlockSpec(memory_space=pltpu.VMEM)] * 2,
            out_specs=[pl.BlockSpec(memory_space=pltpu.HBM)] * 2,
            scratch_shapes=[pltpu.SemaphoreType.DMA((2,))],
            compiler_params=pltpu.CompilerParams(vmem_limit_bytes=8 * 2**20),
        )(ahead, after)

    return jax.shard_map(
        on_device, mesh=mesh, in_specs=(placed,) * 4, out_specs=(placed, placed), check_vma=False
    )
```

```python
import functools

import jax
import jax.numpy as jnp
from jax import lax
from jax.experimental import pallas as pl
from jax.experimental.pallas import tpu as pltpu
from jax.sharding import PartitionSpec as P

MESH = pl.DeviceIdType.MESH

special = (0, 18, 19, 20, 21)
early_runs = ((14, 8), (0, 1))
middle_runs = ((1, 7),)
late_runs = ((8, 6), (22, 3))
runs = early_runs + middle_runs + late_runs
sym_pairs = ((0, 0), (0, 1), (0, 2), (1, 1), (1, 2), (2, 2))
kappa_one = 0.5
damping = 2.0
dissipation = 0.3
time_step = 0.25

LAYERS = 14
ROWS = 32
edge_layers = (1, 2, 11, 12)
y_first = ((0, 8, 0), (14, 8, 8))
y_rest = ((8, 6, 16), (22, 3, 22))


def first_diff(at):
    return ((at(-2) - at(2)) + 8.0 * (at(1) - at(-1))) * (1.0 / 12.0)


def second_diff(at):
    return (16.0 * (at(-1) + at(1)) - (at(-2) + at(2)) - 30.0 * at(0)) * (1.0 / 12.0)


def drift(at, odd_weight, even_weight):
    sums = [at(m) + at(-m) for m in (1, 2, 3)]
    gaps = [at(m) - at(-m) for m in (1, 2, 3)]
    odd = gaps[2] - 6.0 * gaps[1] + 21.0 * gaps[0]
    even = sums[2] - 6.0 * sums[1] + 15.0 * sums[0] - 20.0 * at(0)
    return odd_weight * odd + even_weight * even


def kernel(
    sizes,
    state,
    start,
    before,
    sign,
    ahead,
    after,
    rates,
    first_of,
    before_of,
    cells,
    wrap,
    lean,
    weights,
    diff_y,
    diff_z,
    y_out,
    y_in,
    z_out,
    z_in,
    y_out2,
    y_in2,
    z_out2,
    z_in2,
    edge,
    x_sent,
    x_got,
    n_sent,
    n_got,
    local,
):
    here = {axis: lax.axis_index(axis) for axis in sizes}

    def beside(axis, step):
        return {axis: lax.rem(here[axis] + step + sizes[axis], sizes[axis])}

    barrier = pltpu.get_barrier_semaphore()
    for axis in sizes:
        for step in (1, -1):
            pl.semaphore_signal(barrier, inc=1, device_id=beside(axis, step), device_id_type=MESH)
    own = pltpu.make_async_copy(state, cells.at[:, pl.ds(3, 8), pl.ds(8, 16)], local.at[0])
    own.start()
    leaning = pltpu.make_async_copy(sign, lean, local.at[1])
    leaning.start()
    bases = [
        pltpu.make_async_copy(start, first_of, local.at[2]),
        pltpu.make_async_copy(before, before_of, local.at[3]),
    ]

    def x_copy(side, run):
        first, count = runs[run]
        return pltpu.make_async_remote_copy(
            src_ref=state.at[pl.ds(first, count), pl.ds(0 if side else 5, 3)],
            dst_ref=cells.at[pl.ds(first, count), pl.ds(11 if side else 0, 3), pl.ds(8, 16)],
            send_sem=x_sent.at[side, run],
            recv_sem=x_got.at[side, run],
            device_id=beside("gx", -1 if side else 1),
            device_id_type=MESH,
        )

    def n_copy(which, side):
        axis, out, got = (
            ("gy", y_out.at[side, pl.ds(0, 16)], y_in.at[side, pl.ds(0, 16)]),
            ("gz", z_out.at[side], z_in.at[side]),
            ("gy", y_out2.at[side], y_in2.at[side]),
            ("gz", z_out2.at[side], z_in2.at[side]),
            ("gy", y_out.at[side, pl.ds(16, 9)], y_in.at[side, pl.ds(16, 9)]),
        )[which]
        return pltpu.make_async_remote_copy(
            src_ref=out,
            dst_ref=got,
            send_sem=n_sent.at[which, side],
            recv_sem=n_got.at[which, side],
            device_id=beside(axis, -1 if side else 1),
            device_id_type=MESH,
        )

    def x_start(chosen):
        for run in chosen:
            for side in (0, 1):
                x_copy(side, run).start()

    def x_wait(chosen):
        for run in chosen:
            for side in (0, 1):
                x_copy(side, run).wait_recv()

    def x_left(chosen):
        for run in chosen:
            for side in (0, 1):
                x_copy(side, run).wait_send()

    def n_start(which):
        for side in (0, 1):
            n_copy(which, side).start()

    def n_wait(which):
        for side in (0, 1):
            n_copy(which, side).wait_recv()

    at_early = list(range(len(early_runs)))
    at_middle = list(range(len(early_runs), len(early_runs) + len(middle_runs)))
    at_late = list(range(len(early_runs) + len(middle_runs), len(runs)))

    pl.semaphore_wait(barrier, 2 * len(sizes))
    x_start(at_early[:1])

    own.wait()
    leaning.wait()

    for first, count, at in y_first + y_rest:

        @pl.loop(first, first + count)
        def _(f):
            for r in range(3):
                y_out[0, f - first + at, r] = cells[f, pl.ds(3, 8), 21 + r]
                y_out[1, f - first + at, r] = cells[f, pl.ds(3, 8), 8 + r]

    @pl.loop(0, 25)
    def _(f):
        turned = cells[f, pl.ds(3, 8), pl.ds(8, 16)].reshape(128, 128).T
        z_out[0, f] = turned[120:128]
        z_out[1, f] = turned[0:8]

    n_start(0)
    for f in special:
        for layer in edge_layers:
            cells[f, layer, pl.ds(0, 8)] = jnp.zeros((8, 128), jnp.float32)
            cells[f, layer, pl.ds(24, 8)] = jnp.zeros((8, 128), jnp.float32)
    edge[...] = jnp.zeros_like(edge)

    @pl.loop(0, 8)
    def _(i):
        for k in range(3):
            scaled = cells[19 + k, 3 + i, pl.ds(8, 16)] * (1.0 / 24.0)
            weights[k, i] = scaled
            weights[3 + k, i] = dissipation / 64.0 + jnp.where(lean[k, i] == 1, scaled, -scaled)

    n_start(1)
    low_half = lax.rem(here["gx"], 2) == 0

    @pl.when(low_half)
    def _():
        n_start(4)

    held = at_late[1:]
    x_start([run for run in at_early[1:] + at_middle + at_late if run not in held])

    @pl.when(jnp.logical_not(low_half))
    def _():
        x_start(held)


    lane = lax.broadcasted_iota(jnp.int32, (16, 128), 1)
    lane8 = lax.broadcasted_iota(jnp.int32, (8, 128), 1)

    def along_z(field, layer, start, count):
        inside = cells[field, layer, pl.ds(start, count)]
        outside = wrap[field, layer, pl.ds(start, count)]
        lanes = lane if count == 16 else lane8

        def at(m):
            if m == 0:
                return inside
            if m > 0:
                return pltpu.roll(jnp.where(lanes < m, outside, inside), 128 - m, 1)
            return pltpu.roll(jnp.where(lanes >= 128 + m, outside, inside), -m, 1)

        return at

    def along_y(field, i):
        return lambda m: cells[field, 3 + i, pl.ds(8 + m, 16)]

    def along_x(field, i):
        return lambda m: cells[field, 3 + i + m, pl.ds(8, 16)]

    def turned_back(low, high):
        return jnp.concatenate([high, jnp.zeros((112, 128), jnp.float32), low], axis=0).T

    for copy in bases:
        copy.start()
    n_wait(0)

    def y_place(parts):
        for first, count, at in parts:

            @pl.loop(first, first + count)
            def _(f):
                for r in range(3):
                    cells[f, pl.ds(3, 8), 5 + r] = y_in[0, f - first + at, r]
                    cells[f, pl.ds(3, 8), 24 + r] = y_in[1, f - first + at, r]

    y_place(y_first)

    n_wait(1)

    @pl.loop(0, 25)
    def _(f):
        wrap[f, pl.ds(3, 8), pl.ds(8, 16)] = turned_back(z_in[0, f], z_in[1, f]).reshape(8, 16, 128)

    for first, count, _ in y_first:

        @pl.loop(first, first + count)
        def _(f):
            @pl.loop(0, 8, unroll=4)
            def _(i):
                rates[f, i] = drift(along_y(f, i), weights[1, i], weights[4, i]) + drift(
                    along_z(f, 3 + i, 8, 16), weights[2, i], weights[5, i]
                )

    for first, count, _ in y_rest:

        @pl.loop(first, first + count)
        def _(f):
            @pl.loop(0, 8, unroll=4)
            def _(i):
                rates[f, i] = drift(along_z(f, 3 + i, 8, 16), weights[2, i], weights[5, i])

    x_wait(at_early)

    def of_xy(n, layer, rows):
        if n == 0:
            return 0.5 * cells[0, layer, rows] - cells[18, layer, rows]
        return cells[18 + n, layer, rows]

    for n in range(3):
        for q, layer in enumerate(edge_layers):
            y_out2[0, n, pl.ds(2 * q, 2)] = of_xy(n, layer, pl.ds(22, 2))
            y_out2[1, n, pl.ds(2 * q, 2)] = of_xy(n, layer, pl.ds(8, 2))
    for n, f in enumerate(special):
        y_at = f - 6 if f else 0
        turned = jnp.concatenate(
            [
                cells[f, pl.ds(1, 2), pl.ds(8, 16)].reshape(32, 128),
                cells[f, pl.ds(11, 2), pl.ds(8, 16)].reshape(32, 128),
                y_in[0, y_at, 1],
                y_in[0, y_at, 2],
                y_in[1, y_at, 0],
                y_in[1, y_at, 1],
                jnp.zeros((32, 128), jnp.float32),
            ],
            axis=0,
        ).T
        z_out2[0, n] = turned[120:128]
        z_out2[1, n] = turned[0:8]

    def drift_x(first, count):
        @pl.loop(first, first + count)
        def _(f):
            @pl.loop(0, 8, unroll=2)
            def _(i):
                rates[f, i] += drift(along_x(f, i), weights[0, i], weights[3, i])

    for run in at_early:
        drift_x(*runs[run])

    n_start(2)

    @pl.when(low_half)
    def _():
        x_start(held)

    n_start(3)
    n_wait(3)
    for n, f in enumerate(special):
        back = turned_back(z_in2[0, n], z_in2[1, n])
        wrap[f, pl.ds(1, 2), pl.ds(8, 16)] = back[0:32].reshape(2, 16, 128)
        wrap[f, pl.ds(11, 2), pl.ds(8, 16)] = back[32:64].reshape(2, 16, 128)
        for q, row in enumerate((6, 7, 24, 25)):
            wrap[f, pl.ds(3, 8), row] = back[64 + 8 * q : 72 + 8 * q]
        for layer in range(1, 13):
            diff_y[n, layer] = first_diff(lambda m: cells[f, layer, pl.ds(8 + m, 16)])
            diff_z[n, layer, pl.ds(8, 16)] = first_diff(along_z(f, layer, 8, 16))
        for layer in range(3, 11):
            diff_z[n, layer, pl.ds(0, 8)] = first_diff(along_z(f, layer, 0, 8))
            diff_z[n, layer, pl.ds(24, 8)] = first_diff(along_z(f, layer, 24, 8))

    @pl.loop(0, 8)
    def _(i):
        layer = 3 + i

        def centre(field):
            return cells[field, layer, pl.ds(8, 16)]

        def along(field, k):
            return (along_x(field, i), along_y(field, i), along_z(field, layer, 8, 16))[k]

        def grad(field, k):
            if field in special and k > 0:
                n = special.index(field)
                return diff_y[n, layer] if k == 1 else diff_z[n, layer, pl.ds(8, 16)]
            return first_diff(along(field, k))

        def hess(field, k, l):
            n = special.index(field)
            if k == l:
                return second_diff(along(field, k))
            if (k, l) == (0, 1):
                return first_diff(lambda m: diff_y[n, layer + m])
            if (k, l) == (0, 2):
                return first_diff(lambda m: diff_z[n, layer + m, pl.ds(8, 16)])
            return first_diff(lambda m: diff_z[n, layer, pl.ds(8 + m, 16)])

        def add(field, value):
            rates[field, i] += value

        grad_shift = [[grad(19 + m, k) for k in range(3)] for m in range(3)]
        diverge = grad_shift[0][0] + grad_shift[1][1] + grad_shift[2][2]
        add(0, 2.0 / 3.0 * (centre(7) - diverge))
        for s, (p, q) in enumerate(sym_pairs):
            value = -2.0 * centre(8 + s) + grad_shift[q][p] + grad_shift[p][q]
            if p == q:
                value = value - 2.0 / 3.0 * diverge
            add(1 + s, value)
        add(18, -2.0 * centre(7))
        for p in range(3):
            add(19 + p, 0.75 * centre(22 + p))
        hess_shift = [{pair: hess(19 + m, *pair) for pair in sym_pairs} for m in range(3)]
        for p in range(3):
            lap_shift = hess_shift[p][0, 0] + hess_shift[p][1, 1] + hess_shift[p][2, 2]
            grad_div = hess_shift[0][0, p] + hess_shift[1][min(1, p), max(1, p)] + hess_shift[2][p, 2]
            drive = lap_shift + 1.0 / 3.0 * grad_div
            if p > 0:
                drive = drive - (4.0 / 3.0) * grad(7, p)
            add(14 + p, drive)
            add(22 + p, drive - damping * centre(22 + p))
        hess_chi = {pair: hess(0, *pair) for pair in sym_pairs}
        hess_lapse = {pair: hess(18, *pair) for pair in sym_pairs}
        lap_chi = hess_chi[0, 0] + hess_chi[1, 1] + hess_chi[2, 2]
        lap_lapse = hess_lapse[0, 0] + hess_lapse[1, 1] + hess_lapse[2, 2]
        add(7, -lap_lapse + kappa_one * centre(17))
        grad_gamma = [[grad(14 + m, k) for k in range(3)] for m in range(3)]
        ricci = []
        for s, (p, q) in enumerate(sym_pairs):
            lap_metric = second_diff(along(1 + s, 1)) + second_diff(along(1 + s, 2))
            value = -0.5 * lap_metric + 0.5 * (grad_gamma[q][p] + grad_gamma[p][q]) + 0.5 * hess_chi[p, q]
            if p == q:
                value = value + 0.5 * lap_chi
            ricci.append(value)
        bare = [ricci[s] - hess_lapse[pair] for s, pair in enumerate(sym_pairs)]
        trace = bare[0] + bare[3] + bare[5]
        for s, (p, q) in enumerate(sym_pairs):
            add(8 + s, bare[s] - 1.0 / 3.0 * trace if p == q else bare[s])
        add(17, 0.5 * (ricci[0] + ricci[3] + ricci[5]) - 2.0 * kappa_one * centre(17))

    x_wait(at_middle)
    for run in at_middle:
        drift_x(*runs[run])

    @pl.loop(0, 8)
    def _(i):
        bent = [-0.5 * second_diff(along_x(1 + s, i)) for s in range(6)]
        trace = bent[0] + bent[3] + bent[5]
        for s, (p, q) in enumerate(sym_pairs):
            rates[8 + s, i] += bent[s] - 1.0 / 3.0 * trace if p == q else bent[s]
        rates[17, i] += 0.5 * trace
        slope = -(4.0 / 3.0) * first_diff(along_x(7, i))
        rates[14, i] += slope
        rates[22, i] += slope

    for copy in bases:
        copy.wait()

    def finish(f, i, value):
        ahead[f, i] = first_of[f, i] + time_step / 2.0 * value
        after[f, i] = before_of[f, i] + time_step / 3.0 * value

    for run in at_early + at_middle:
        first, count = runs[run]

        @pl.loop(first, first + count)
        def _(f):
            @pl.loop(0, 8, unroll=4)
            def _(i):
                finish(f, i, rates[f, i])

    @pl.when(jnp.logical_not(low_half))
    def _():
        x_left(at_early + at_middle + at_late[:1])
        n_start(4)

    n_wait(4)
    y_place(y_rest)
    for first, count, _ in y_rest:

        @pl.loop(first, first + count)
        def _(f):
            @pl.loop(0, 8, unroll=8)
            def _(i):
                rates[f, i] += drift(along_y(f, i), weights[1, i], weights[4, i])

    def close(run, together):
        x_wait([run])
        first, count = runs[run]

        @pl.loop(first, first + count)
        def _(f):
            @pl.loop(0, 8, unroll=together)
            def _(i):
                finish(f, i, rates[f, i] + drift(along_x(f, i), weights[0, i], weights[3, i]))

    close(at_late[0], 4)
    n_wait(2)

    def corner(n):
        for q in range(4):
            edge[n, q, pl.ds(6, 2)] = y_in2[0, n, pl.ds(2 * q, 2)]
            edge[n, q, pl.ds(24, 2)] = y_in2[1, n, pl.ds(2 * q, 2)]
        outer, inner, beyond, last = [
            first_diff(lambda m: edge[n, q, pl.ds(8 + m, 16)]) * (1.0 / 12.0) for q in range(4)
        ]
        return ((0, outer - 8.0 * inner), (1, inner), (6, -beyond), (7, 8.0 * beyond - last))

    for n, (fields, factor) in enumerate((((9,), 1.0), ((15, 23), 1.0 / 3.0), ((14, 22), 1.0 / 3.0))):
        for i, value in corner(n):
            for f in fields:
                if f > 21:
                    rates[f, i] += factor * value
                else:
                    ahead[f, i] += (time_step / 2.0 * factor) * value
                    after[f, i] += (time_step / 3.0 * factor) * value

    close(at_late[1], 8)

    @pl.when(low_half)
    def _():
        x_left(at_early + at_middle + at_late[:1])

    x_left([run for run in range(len(runs)) if run not in at_early + at_middle + at_late[:1]])
    for which in range(5):
        for side in (0, 1):
            n_copy(which, side).wait_send()


def section_of(sizes, *arrays):
    block = (8, 16, 128)
    f32 = jnp.float32
    whole = jax.ShapeDtypeStruct((25,) + block, f32)
    return pl.pallas_call(
        functools.partial(kernel, sizes),
        out_shape=(whole, whole),
        in_specs=[pl.BlockSpec(memory_space=pltpu.HBM)] * 4,
        out_specs=[pl.BlockSpec(memory_space=pltpu.VMEM)] * 2,
        scratch_shapes=[
            pltpu.VMEM((25,) + block, f32),
            pltpu.VMEM((25,) + block, f32),
            pltpu.VMEM((25,) + block, f32),
            pltpu.VMEM((25, LAYERS, ROWS, 128), f32),
            pltpu.VMEM((25, LAYERS, ROWS, 128), f32),
            pltpu.VMEM((3,) + block, jnp.int32),
            pltpu.VMEM((6,) + block, f32),
            pltpu.VMEM((5, LAYERS, 16, 128), f32),
            pltpu.VMEM((5, LAYERS, ROWS, 128), f32),
            pltpu.VMEM((2, 25, 3, 8, 128), f32),
            pltpu.VMEM((2, 25, 3, 8, 128), f32),
            pltpu.VMEM((2, 25, 8, 128), f32),
            pltpu.VMEM((2, 25, 8, 128), f32),
            pltpu.VMEM((2, 3, 8, 128), f32),
            pltpu.VMEM((2, 3, 8, 128), f32),
            pltpu.VMEM((2, 5, 8, 128), f32),
            pltpu.VMEM((2, 5, 8, 128), f32),
            pltpu.VMEM((3, 4, ROWS, 128), f32),
            pltpu.SemaphoreType.DMA((2, len(runs))),
            pltpu.SemaphoreType.DMA((2, len(runs))),
            pltpu.SemaphoreType.DMA((5, 2)),
            pltpu.SemaphoreType.DMA((5, 2)),
            pltpu.SemaphoreType.DMA((4,)),
        ],
        compiler_params=pltpu.CompilerParams(
            collective_id=0, has_side_effects=True, vmem_limit_bytes=40 * 2**20
        ),
    )(*(pltpu.with_memory_space_constraint(x, pltpu.HBM) for x in arrays))


def put_out(ahead, after, ahead_out, after_out, sems):
    copies = [
        pltpu.make_async_copy(ahead, ahead_out, sems.at[0]),
        pltpu.make_async_copy(after, after_out, sems.at[1]),
    ]
    for copy in copies:
        copy.start()
    for copy in copies:
        copy.wait()


def solution(mesh):
    placed = P(None, "gx", "gy", "gz")
    sizes = dict(mesh.shape)

    def on_device(section_state, step_start, weighted_sum, upwind_sign):
        ahead, after = section_of(sizes, section_state, step_start, weighted_sum, upwind_sign)
        return pl.pallas_call(
            put_out,
            out_shape=(ahead, after),
            in_specs=[pl.BlockSpec(memory_space=pltpu.VMEM)] * 2,
            out_specs=[pl.BlockSpec(memory_space=pltpu.HBM)] * 2,
            scratch_shapes=[pltpu.SemaphoreType.DMA((2,))],
            compiler_params=pltpu.CompilerParams(vmem_limit_bytes=8 * 2**20),
        )(ahead, after)

    return jax.shard_map(
        on_device, mesh=mesh, in_specs=(placed,) * 4, out_specs=(placed, placed), check_vma=False
    )
```
